32 devices in a mesh: grp: 2 (over y), res: 8 (over z, x), seq: 2 (over core).
Axes of the slice: x: 2, y: 2, z: 4, core: 2. Of those that a mesh axis runs over, the one named last changes fastest.
Arguments:
- aligned_activity: bfloat16 [512, 512, 256], P(('grp', 'seq'), 'res'), parts along dimension 0, may hold values from -6 to 6
- pair_state: bfloat16 [1024, 512, 128], P(('grp', 'res'), 'seq'), parts along dimension 0, may hold values from -6 to 6
- focus_scaling_vector: float32 [256], replicated, may hold values from 0.5 to 2
- combined_probe_matrix: bfloat16 [256, 1024], replicated, may hold values from -0.375 to 0.375
- sigmoid_offset_vector: float32 [256], replicated, may hold values from -4 to 4
- focus_final_matrix: bfloat16 [256, 256], replicated, may hold values from -0.375 to 0.375
- pair_norm_gain: float32 [128], replicated, may hold values from 0.5 to 2
- pair_bias_matrix: float32 [128, 8], replicated, may hold values from -36 to 36
- feedforward_scaling_vector: float32 [256], replicated, may hold values from 0.5 to 2
- feedforward_widen_matrix: bfloat16 [256, 1024], replicated, may hold values from -0.375 to 0.375
- feedforward_shrink_matrix: bfloat16 [1024, 256], replicated, may hold values from -0.1875 to 0.1875
- tensor_scaling_vector: float32 [256], replicated, may hold values from 0.5 to 2
- twin_operand_matrix: bfloat16 [256, 64], replicated, may hold values from -0.375 to 0.375
- tensor_final_matrix: bfloat16 [1024, 128], replicated, may hold values from -3 to 3
Outputs:
- alignment_output: bfloat16 [512, 512, 256], P(('grp', 'seq'), 'res'), parts along dimension 0
- pair_output: bfloat16 [1024, 512, 128], P(('grp', 'res'), 'seq'), parts along dimension 0
The draws below stay inside these ranges and needn't reach their ends.
There are 2 independent parts, one for each index of `grp`. The reference program is written for one: setup_inputs(seed, part) draws one part's arguments, and reference() takes and returns one part's arrays. A program takes and returns all parts, laid end to end along the dimension named above; an argument that names none is the same for every part. Nothing has to cross between parts.
All inputs are finite; a program needn't handle non-finite values.
Results may differ from the reference program's by a relative error of at most 0.0095.
The reference program's roundings to bfloat16 on the way count: a program that leaves them out, or rounds other values in their place, can miss the bound.
Values may be sent and summed in bfloat16 or wider, within the bound.
A program may use at most 256 MiB of HBM per device.

```python
import math
import jax
import jax.numpy as jnp
from jax import lax

ALIGNED_DEPTH = 256
COUPLING_DEPTH = 128
FOCUS_GROUPS = 8
PRODUCT_DEPTH = 32
ALIGNED_CHAINS = 256
AMINO_SITES = 512
HIDDEN_UNITS = 1024
N_RES = 8


def draw_pair_bias_matrix(key, part):
    raw = jnp.clip(jax.random.normal(key, (COUPLING_DEPTH, FOCUS_GROUPS), jnp.float32), -4.0, 4.0)
    return raw * 0.09


def level_of(rng, shape, split, low, largest):
    gain = 1.0
    for position, parts in split:
        steps = jax.random.uniform(jax.random.fold_in(jax.random.fold_in(rng, 6), position), (parts,), jnp.float32, low / len(split), largest / len(split))
        gain = gain * jnp.repeat(jnp.exp(steps), shape[position] // parts).reshape((-1,) + (1,) * (len(shape) - 1 - position))
    return gain


def normal_values(own_key, extent, width, reach, split=(), held_as=jnp.bfloat16):
    entries = jax.random.normal(own_key, extent, jnp.float32) * width
    if len(split) > 0:
        entries = level_of(own_key, extent, split, -0.22, 0.18) * entries
    return jnp.clip(entries, min=-reach, max=reach).astype(held_as)


def setup_inputs(seed: int = 0, part: int = 0) -> dict:
    splits = jax.random.split(jax.random.key(seed), 15)
    own_keys = jax.random.split(jax.random.fold_in(splits[14], part), 15)
    aligned_activity = normal_values(own_keys[0], (ALIGNED_CHAINS, AMINO_SITES, ALIGNED_DEPTH), 1.0, 6.0, ((0, 2), (1, 8)))
    pair_state = normal_values(own_keys[1], (AMINO_SITES, AMINO_SITES, COUPLING_DEPTH), 1.0, 6.0, ((0, 8), (1, 2)))
    focus_scaling_vector = jnp.clip(jnp.exp(jax.random.uniform(splits[2], (ALIGNED_DEPTH,), jnp.float32, math.log(0.5), math.log(2.0))), 0.5, 2.0)
    combined_probe_matrix = normal_values(splits[3], (ALIGNED_DEPTH, 4 * ALIGNED_DEPTH), ALIGNED_DEPTH ** -0.5, 0.375)
    sigmoid_offset_vector = normal_values(splits[4], (ALIGNED_DEPTH,), 1.0, 4.0, (), jnp.float32)
    focus_final_matrix = normal_values(splits[5], (ALIGNED_DEPTH, ALIGNED_DEPTH), ALIGNED_DEPTH ** -0.5, 0.375)
    pair_norm_gain = jnp.clip(jnp.exp(jax.random.uniform(splits[6], (COUPLING_DEPTH,), jnp.float32, math.log(0.5), math.log(2.0))), 0.5, 2.0)
    pair_bias_matrix = draw_pair_bias_matrix(jax.random.fold_in(splits[14], 71), part)
    feedforward_scaling_vector = jnp.clip(jnp.exp(jax.random.uniform(splits[8], (ALIGNED_DEPTH,), jnp.float32, math.log(0.5), math.log(2.0))), 0.5, 2.0)
    feedforward_widen_matrix = normal_values(splits[9], (ALIGNED_DEPTH, HIDDEN_UNITS), ALIGNED_DEPTH ** -0.5, 0.375)
    feedforward_shrink_matrix = normal_values(splits[10], (HIDDEN_UNITS, ALIGNED_DEPTH), HIDDEN_UNITS ** -0.5, 0.1875)
    tensor_scaling_vector = jnp.clip(jnp.exp(jax.random.uniform(splits[11], (ALIGNED_DEPTH,), jnp.float32, math.log(0.5), math.log(2.0))), 0.5, 2.0)
    twin_operand_matrix = normal_values(splits[12], (ALIGNED_DEPTH, 2 * PRODUCT_DEPTH), ALIGNED_DEPTH ** -0.5, 0.375)
    tensor_final_matrix = normal_values(splits[13], (PRODUCT_DEPTH * PRODUCT_DEPTH, COUPLING_DEPTH), (max(1, PRODUCT_DEPTH * PRODUCT_DEPTH // ALIGNED_CHAINS)) ** -0.5, 3.0)
    return dict(aligned_activity=aligned_activity, pair_state=pair_state, focus_scaling_vector=focus_scaling_vector, combined_probe_matrix=combined_probe_matrix, sigmoid_offset_vector=sigmoid_offset_vector, focus_final_matrix=focus_final_matrix, pair_norm_gain=pair_norm_gain, pair_bias_matrix=pair_bias_matrix, feedforward_scaling_vector=feedforward_scaling_vector, feedforward_widen_matrix=feedforward_widen_matrix, feedforward_shrink_matrix=feedforward_shrink_matrix, tensor_scaling_vector=tensor_scaling_vector, twin_operand_matrix=twin_operand_matrix, tensor_final_matrix=tensor_final_matrix)


def layer_normalize(inputs, scale_gain):
    sample_expectation = lax.optimization_barrier(jnp.mean(inputs, axis=-1, keepdims=True))
    centered = inputs - sample_expectation
    variance = lax.optimization_barrier(jnp.mean(centered * centered, axis=-1, keepdims=True))
    return centered * lax.rsqrt(variance + 1e-05) * scale_gain

def reference(aligned_activity, pair_state, focus_scaling_vector, combined_probe_matrix, sigmoid_offset_vector, focus_final_matrix, pair_norm_gain, pair_bias_matrix, feedforward_scaling_vector, feedforward_widen_matrix, feedforward_shrink_matrix, tensor_scaling_vector, twin_operand_matrix, tensor_final_matrix):
    subspace_depth = ALIGNED_DEPTH // FOCUS_GROUPS
    probe_multiplier = subspace_depth ** (-0.5)
    pair_norm = layer_normalize(pair_state.astype(jnp.float32), pair_norm_gain)
    pair_bias = jnp.einsum('ijc,ch->hij', pair_norm, pair_bias_matrix, precision=lax.Precision.HIGHEST).astype(jnp.bfloat16)
    bias_wide = pair_bias.astype(jnp.float32)

    def row_attention_update(sequence):
        residual_state = sequence.astype(jnp.float32)
        normalized_rows = layer_normalize(residual_state, focus_scaling_vector).astype(jnp.bfloat16)
        mapped_entries = jnp.dot(normalized_rows, combined_probe_matrix, preferred_element_type=jnp.float32)
        probe_entries = (mapped_entries[:, :ALIGNED_DEPTH] * probe_multiplier).astype(jnp.bfloat16).reshape(AMINO_SITES, FOCUS_GROUPS, subspace_depth)
        lookup_entries = mapped_entries[:, ALIGNED_DEPTH:2 * ALIGNED_DEPTH].astype(jnp.bfloat16).reshape(AMINO_SITES, FOCUS_GROUPS, subspace_depth)
        content_entries = mapped_entries[:, 2 * ALIGNED_DEPTH:3 * ALIGNED_DEPTH].astype(jnp.bfloat16).reshape(AMINO_SITES, FOCUS_GROUPS, subspace_depth)
        sigmoid_filter = jax.nn.sigmoid(mapped_entries[:, 3 * ALIGNED_DEPTH:] + sigmoid_offset_vector)
        scores = jnp.einsum('ihd,jhd->hij', probe_entries.astype(jnp.float32), lookup_entries.astype(jnp.float32)) + bias_wide
        top_score = lax.optimization_barrier(jnp.max(scores, axis=-1, keepdims=True))
        exponent = jnp.exp(scores - top_score)
        softmax_shares = (exponent / lax.optimization_barrier(jnp.sum(exponent, axis=-1, keepdims=True))).astype(jnp.bfloat16)
        mixed_entries = jnp.einsum('tnx,xtq->ntq', softmax_shares.astype(jnp.float32), content_entries.astype(jnp.float32)).reshape(AMINO_SITES, ALIGNED_DEPTH)
        gated_rows = (mixed_entries * sigmoid_filter).astype(jnp.bfloat16)
        residual_state = residual_state + jnp.dot(gated_rows, focus_final_matrix, preferred_element_type=jnp.float32)
        normalized_rows = layer_normalize(residual_state, feedforward_scaling_vector).astype(jnp.bfloat16)
        hidden = jnp.maximum(jnp.dot(normalized_rows, feedforward_widen_matrix, preferred_element_type=jnp.float32), 0.0).astype(jnp.bfloat16)
        residual_state = residual_state + jnp.dot(hidden, feedforward_shrink_matrix, preferred_element_type=jnp.float32)
        updated_state = residual_state.astype(jnp.bfloat16)
        normalized_rows = layer_normalize(updated_state.astype(jnp.float32), tensor_scaling_vector).astype(jnp.bfloat16)
        left_right_factors = jnp.dot(normalized_rows, twin_operand_matrix, preferred_element_type=jnp.float32).astype(jnp.bfloat16)
        return (updated_state, left_right_factors)
    alignment_output, left_right_factors = lax.map(row_attention_update, aligned_activity)
    left_fac = left_right_factors[:, :, :PRODUCT_DEPTH].astype(jnp.float32)
    right_fac = left_right_factors[:, :, PRODUCT_DEPTH:].astype(jnp.float32)
    row_block = AMINO_SITES // N_RES
    out_table = tensor_final_matrix.astype(jnp.float32).reshape(PRODUCT_DEPTH, PRODUCT_DEPTH, COUPLING_DEPTH)

    def pair_rows(block_index):
        left_rows = lax.dynamic_slice_in_dim(left_fac, block_index * row_block, row_block, 1)
        tensor_total = jnp.einsum('sic,sje->icje', left_rows, right_fac, precision=lax.Precision.HIGHEST)
        sample_expectation = (tensor_total / ALIGNED_CHAINS).astype(jnp.bfloat16)
        return jnp.einsum('icje,cez->ijz', sample_expectation.astype(jnp.float32), out_table, precision=lax.Precision.HIGHEST)
    update = lax.map(pair_rows, jnp.arange(N_RES, dtype=jnp.int32)).reshape(AMINO_SITES, AMINO_SITES, COUPLING_DEPTH)
    pair_output = (pair_state.astype(jnp.float32) + update).astype(jnp.bfloat16)
    return (alignment_output, pair_output)
```

```python
import functools
import math

import jax
import jax.numpy as jnp
from jax import lax
from jax.experimental import pallas as pl
from jax.experimental.pallas import tpu as pltpu
from jax.sharding import PartitionSpec as P

LOG2E = math.log2(math.e)
VMEM_LIMIT = 60 * 1024 * 1024
FUSED_VMEM = 67043328
CHUNKS = 4
GROUPS = 2


def layer_normalize(inputs, scale_gain):
    sample_expectation = jnp.mean(inputs, axis=-1, keepdims=True)
    centered = inputs - sample_expectation
    variance = jnp.mean(centered * centered, axis=-1, keepdims=True)
    return centered * lax.rsqrt(variance + 1e-05) * scale_gain


def dot_f32(a, b, ca, cb):
    return lax.dot_general(a, b, (((ca,), (cb,)), ((), ())), preferred_element_type=jnp.float32)


def sequence_kernel(
    heads,
    pack,
    blocks,
    *refs,
):
    rank_ref, refs = refs[0], refs[1:]
    x_refs, refs = refs[:blocks], refs[blocks:]
    weight_refs, refs = refs[:11], refs[11:]
    out_refs, (right_ref, gathered, left_acc, right_acc) = refs[:blocks], refs[blocks:]
    (
        bias_ref,
        gain_ref,
        probe_ref,
        offset_ref,
        final_ref,
        ff_gain_ref,
        widen_ref,
        shrink_ref,
        opm_gain_ref,
        left_w_ref,
        right_w_ref,
    ) = weight_refs
    rank = rank_ref[0]
    step = pl.program_id(0)
    steps = right_ref.shape[2]
    _, rows, width = x_refs[0].shape
    length = blocks * rows
    depth = width // heads
    for d in range(blocks):
        gathered[lax.rem(rank + blocks - d, blocks)] = x_refs[d][0]
    x = gathered[...].astype(jnp.float32).reshape(length, width)
    normed = layer_normalize(x, gain_ref[...]).astype(jnp.bfloat16)
    mapped = dot_f32(probe_ref[...], normed, 1, 1)
    q = (mapped[:width] * (depth ** (-0.5) * LOG2E)).astype(jnp.bfloat16)
    k = mapped[width : 2 * width].astype(jnp.bfloat16)
    v = mapped[2 * width : 3 * width].astype(jnp.bfloat16)
    gate = jax.nn.sigmoid(mapped[3 * width :] + offset_ref[...])
    ones = jnp.ones((16, length), jnp.bfloat16)
    gated = []
    for h in range(heads):
        part = slice(h * depth, (h + 1) * depth)
        scores = dot_f32(k[part], q[part], 0, 0) + bias_ref[h]
        top = jnp.max(scores, axis=0, keepdims=True)
        p = jnp.exp2(scores - top).astype(jnp.bfloat16)
        mixed = dot_f32(jnp.concatenate([v[part], ones], axis=0), p, 1, 0)
        share = mixed[:depth] / mixed[depth : depth + 1]
        gated.append((share * gate[part]).astype(jnp.bfloat16))
    gated = jnp.concatenate(gated, axis=0)
    stream = x + dot_f32(gated, final_ref[...], 0, 0)
    normed = layer_normalize(stream, ff_gain_ref[...]).astype(jnp.bfloat16)
    hidden = jnp.maximum(dot_f32(normed, widen_ref[...], 1, 0), 0.0).astype(jnp.bfloat16)
    stream = stream + dot_f32(hidden, shrink_ref[...], 1, 0)
    updated = stream.astype(jnp.bfloat16)
    gathered[...] = stream.reshape(blocks, rows, width).astype(jnp.bfloat16)
    for d in range(blocks):
        out_refs[d][step] = gathered[lax.rem(rank + d, blocks)]
    normed = layer_normalize(updated.astype(jnp.float32), opm_gain_ref[...]).astype(jnp.bfloat16)
    slot = lax.rem(step, pack)
    left = dot_f32(normed, left_w_ref[slot], 1, 0).reshape(left_acc.shape)

    @pl.when(slot == 0)
    def _():
        left_acc[...] = left

    @pl.when(slot != 0)
    def _():
        left_acc[...] = left_acc[...] + left

    factor = right_w_ref.shape[0]
    right = dot_f32(right_w_ref[...], normed, 1, 1)
    for e in range(factor):
        right_acc[e, pl.ds(step, 1), :] = right[e : e + 1]

    @pl.when(step == steps - 1)
    def _():
        lanes = left_acc.shape[2]
        cols = right_ref.shape[3]
        for part in range(right_ref.shape[0]):
            right_ref[part] = right_acc[:, :, part * cols : (part + 1) * cols].astype(jnp.bfloat16)
        for d in range(blocks):
            if lanes < width:
                out_refs[d][steps] = jnp.zeros((rows, width), jnp.bfloat16)
            out_refs[d][steps, :, :lanes] = left_acc[lax.rem(rank + d, blocks)].astype(jnp.bfloat16)


def run_sequences(rank, xs, bias, weights, heads, pack, halves):
    blocks = len(xs)
    steps, rows, width = xs[0].shape
    length = blocks * rows
    factor = weights[-1].shape[0]
    cols = length // halves
    whole = lambda a: pl.BlockSpec(
        a.shape, lambda s, n=a.ndim: (0,) * n, pipeline_mode=pl.Buffered(1)
    )
    kept = lambda shape: pl.BlockSpec(shape, lambda s, n=len(shape): (0,) * n)
    lanes = pack * factor
    hidden = weights[5].shape[1]
    flops = 2 * length * width * (5 * width + 2 * hidden + 128) + 4 * length * length * width
    shapes = [(steps + 1, rows, width)] * blocks + [(halves, factor, steps, cols)]
    return pl.pallas_call(
        functools.partial(sequence_kernel, heads, pack, blocks),
        grid=(steps,),
        in_specs=[pl.BlockSpec(memory_space=pltpu.SMEM)]
        + [pl.BlockSpec((1, rows, width), lambda s: (s, 0, 0)) for _ in xs]
        + [whole(a) for a in (bias,) + weights],
        out_specs=[kept(a) for a in shapes],
        out_shape=[jax.ShapeDtypeStruct(a, jnp.bfloat16) for a in shapes],
        scratch_shapes=[
            pltpu.VMEM((blocks, rows, width), jnp.bfloat16),
            pltpu.VMEM((blocks, rows, lanes), jnp.float32),
            pltpu.VMEM((factor, steps, length), jnp.float32),
        ],
        compiler_params=pltpu.CompilerParams(
            dimension_semantics=("arbitrary",), vmem_limit_bytes=VMEM_LIMIT
        ),
        cost_estimate=pl.CostEstimate(
            flops=steps * flops * 3,
            bytes_accessed=bias.size * 4 + 4 * length * width * steps,
            transcendentals=steps * heads * length * length,
        ),
        name="sequences",
    )(rank, *xs, bias, *weights)


def deal_kernel(chunks, rank_ref, x_ref, *out_refs):
    blocks = x_ref.shape[0]
    part = x_ref.shape[1] // chunks
    for c in range(chunks):
        for d in range(blocks):
            source = lax.rem(rank_ref[0] + d, blocks)
            out_refs[c * blocks + d][...] = x_ref[source, c * part : (c + 1) * part]


def collect_kernel(chunks, rank_ref, *refs):
    in_refs, (out_ref, left_ref) = refs[:-2], refs[-2:]
    blocks = out_ref.shape[0]
    part = out_ref.shape[1] // chunks
    lanes = left_ref.shape[3]
    for c in range(chunks):
        for d in range(blocks):
            target = lax.rem(rank_ref[0] + blocks - d, blocks)
            y_ref = in_refs[c * blocks + d]
            out_ref[target, c * part : (c + 1) * part] = y_ref[:part]
            left_ref[target, c] = y_ref[part, :, :lanes]


def vmem_call(kernel, shapes, rank, arrays, name):
    return pl.pallas_call(
        kernel,
        in_specs=[pl.BlockSpec(memory_space=pltpu.SMEM)]
        + [pl.BlockSpec(memory_space=pltpu.VMEM)] * len(arrays),
        out_specs=[pl.BlockSpec(memory_space=pltpu.VMEM)] * len(shapes),
        out_shape=[jax.ShapeDtypeStruct(a, jnp.bfloat16) for a in shapes],
        compiler_params=pltpu.CompilerParams(vmem_limit_bytes=VMEM_LIMIT // 2),
        cost_estimate=pl.CostEstimate(
            flops=0, bytes_accessed=4 * sum(a.size for a in arrays), transcendentals=0
        ),
        name=name,
    )(rank, *arrays)


def shift_all(arrays):
    size = len(arrays)
    return [arrays[0]] + [
        lax.ppermute(arrays[d], "res", [(r, (r + d) % size) for r in range(size)])
        for d in range(1, size)
    ]


def product_kernel(rows, seq_total, left_ref, *refs):
    right_refs, (table_ref, pair_ref, out_ref, stack) = refs[:-4], refs[-4:]
    groups, factor, part, cols = right_refs[0].shape
    scale = 1.0 / seq_total
    left = left_ref[...]
    for e in range(factor):
        right = jnp.concatenate(
            [ref[:, e].reshape(groups * part, cols) for ref in right_refs], axis=0
        )
        outer = (dot_f32(left, right, 1, 0) * scale).astype(jnp.bfloat16)
        stack[:, e * factor : (e + 1) * factor, :] = outer.reshape(rows, factor, cols)
    for i in range(rows):
        update = dot_f32(table_ref[...], stack[i], 1, 0)
        out_ref[i] = (pair_ref[i].astype(jnp.float32) + update.T).astype(jnp.bfloat16)


def run_product(left, rights, table, pair):
    total_rows, seq_total = left.shape
    _, factor, _, cols = rights[0].shape
    pair_rows = pair.shape[0]
    rows = math.gcd(pair_rows, 8)
    width = pair.shape[2]
    return pl.pallas_call(
        functools.partial(product_kernel, rows, seq_total),
        grid=(pair_rows // rows,),
        in_specs=[
            pl.BlockSpec((rows * factor, seq_total), lambda b: (b, 0)),
            *[
                pl.BlockSpec(a.shape, lambda b: (0, 0, 0, 0), pipeline_mode=pl.Buffered(1))
                for a in rights
            ],
            pl.BlockSpec(table.shape, lambda b: (0, 0), pipeline_mode=pl.Buffered(1)),
            pl.BlockSpec((rows, cols, width), lambda b: (b, 0, 0)),
        ],
        out_specs=pl.BlockSpec((rows, cols, width), lambda b: (b, 0, 0)),
        out_shape=jax.ShapeDtypeStruct(pair.shape, jnp.bfloat16),
        scratch_shapes=[pltpu.VMEM((rows, factor * factor, cols), jnp.bfloat16)],
        compiler_params=pltpu.CompilerParams(
            dimension_semantics=("arbitrary",), vmem_limit_bytes=VMEM_LIMIT
        ),
        cost_estimate=pl.CostEstimate(
            flops=4 * total_rows * cols * factor * (seq_total + width),
            bytes_accessed=2 * (left.size * (1 + cols * factor // total_rows) + left.size + 2 * pair.size),
            transcendentals=0,
        ),
        name="product",
    )(left, *rights, table, pair)


def permuted_on_device(
    aligned_activity,
    pair_state,
    focus_scaling_vector,
    combined_probe_matrix,
    sigmoid_offset_vector,
    focus_final_matrix,
    pair_norm_gain,
    pair_bias_matrix,
    feedforward_scaling_vector,
    feedforward_widen_matrix,
    feedforward_shrink_matrix,
    tensor_scaling_vector,
    twin_operand_matrix,
    tensor_final_matrix,
):
    width = aligned_activity.shape[2]
    heads = pair_bias_matrix.shape[1]
    factor = twin_operand_matrix.shape[1] // 2
    res_axis = lax.axis_size("res")
    seq_axis = lax.axis_size("seq")
    rows = aligned_activity.shape[1]
    seq_count = aligned_activity.shape[0] // res_axis
    length = rows * res_axis
    col_block = pair_state.shape[1]
    chunks = math.gcd(CHUNKS, seq_count)
    per_chunk = seq_count // chunks
    pack = per_chunk

    groups = math.gcd(GROUPS, chunks) if seq_count % (8 * GROUPS) == 0 else 1
    rank = lax.axis_index("res").astype(jnp.int32).reshape(1)
    pieces = aligned_activity.reshape(res_axis, seq_count, rows, width)
    dealt = vmem_call(
        functools.partial(deal_kernel, chunks),
        [(per_chunk, rows, width)] * (chunks * res_axis),
        rank,
        [pieces],
        "deal",
    )
    arrived = [shift_all(dealt[c * res_axis : (c + 1) * res_axis]) for c in range(chunks)]

    pair_norm = layer_normalize(pair_state.astype(jnp.float32), pair_norm_gain)
    bias_tile = jnp.einsum(
        "ijc,ch->hij", pair_norm, pair_bias_matrix, precision=lax.Precision.HIGHEST
    ).astype(jnp.bfloat16)
    bias_rows = lax.all_gather(bias_tile, "res", axis=1, tiled=True)
    bias_all = lax.all_gather(bias_rows, "seq", axis=0)
    bias = bias_all.transpose(1, 0, 3, 2).reshape(heads, length, length)
    bias = bias.astype(jnp.float32) * LOG2E

    left_w = twin_operand_matrix[:, :factor]
    left_w = jnp.stack(
        [jnp.pad(left_w, ((0, 0), (t * factor, (pack - 1 - t) * factor))) for t in range(pack)]
    )
    weights = (
        focus_scaling_vector.reshape(1, -1),
        combined_probe_matrix.T,
        sigmoid_offset_vector.reshape(-1, 1),
        focus_final_matrix,
        feedforward_scaling_vector.reshape(1, -1),
        feedforward_widen_matrix,
        feedforward_shrink_matrix,
        tensor_scaling_vector.reshape(1, -1),
        left_w,
        twin_operand_matrix[:, factor:].T,
    )
    returned, rights, pending = [], [], []
    for c in range(chunks):
        *updated, right = run_sequences(rank, arrived[c], bias, weights, heads, pack, seq_axis)
        returned += shift_all(updated)
        pending.append(right)
        if len(pending) == chunks // groups:
            right = jnp.concatenate(pending, axis=2)
            right = lax.all_to_all(right, "seq", split_axis=0, concat_axis=0, tiled=True)
            rights.append(lax.all_gather(right, "res", axis=0, tiled=True))
            pending = []
    if (seq_count // groups) % 8 != 0:
        rights = [r.transpose(1, 0, 2, 3).reshape(1, factor, -1, col_block) for r in rights]
    alignment_output, left = vmem_call(
        functools.partial(collect_kernel, chunks),
        [pieces.shape, (res_axis, chunks, rows, pack * factor)],
        rank,
        returned,
        "collect",
    )
    alignment_output = alignment_output.reshape(aligned_activity.shape)
    left = lax.all_gather(left, "seq", axis=0)
    left = left.reshape(seq_axis, res_axis, groups, chunks // groups, rows, pack, factor)
    left = left.transpose(4, 6, 2, 1, 0, 3, 5).reshape(rows * factor, -1)

    table = tensor_final_matrix.reshape(factor, factor, -1).transpose(2, 1, 0)
    table = table.reshape(table.shape[0], -1)
    pair_output = run_product(left, rights, table, pair_state)
    return (alignment_output, pair_output)


MESH = pl.DeviceIdType.MESH
GROUP = 8
AHEAD = 6
RETURNS = 4
LANES = 128


def dot_t(a, b):
    return dot_f32(a, b, 1, 1)


def wait_for(ref, sem):
    pltpu.make_async_copy(ref, ref, sem).wait()


def send(src, dst, sent, arrived, **peer):
    pltpu.make_async_remote_copy(
        src_ref=src,
        dst_ref=dst,
        send_sem=sent,
        recv_sem=arrived,
        device_id=peer,
        device_id_type=MESH,
    ).start()


class Relay:
    def __init__(self, rank, deep, wide, tile, tiles, arrived, sent_z, sent_x, forward=None):
        self.rank, self.deep, self.wide = rank, deep, wide
        self.z, self.x = rank // wide, rank % wide
        self.tile, self.tiles, self.arrived = tile, tiles, arrived
        self.sent_z, self.sent_x, self.forward = sent_z, sent_x, forward

    def pass_on(self, owner):
        for d in range(1, self.wide):
            peer = self.z * self.wide + (self.x + d) % self.wide
            send(self.tile(owner), self.tile(owner), self.sent_x, self.arrived.at[owner], res=peer)
        if self.forward is not None:
            self.forward(owner)

    def ends(self, hop, way):
        z = self.z - hop if way == 0 else self.z + hop
        there = z >= 0 if way == 0 else z < self.deep
        onward = self.z + 1 < self.deep if way == 0 else self.z >= 1
        peer = self.rank + self.wide if way == 0 else self.rank - self.wide
        return z * self.wide + self.x, there, onward, peer

    def start(self):
        for way in range(2):
            owner, _, onward, peer = self.ends(0, way)

            @pl.when(onward)
            def _():
                send(
                    self.tile(self.rank),
                    self.tile(self.rank),
                    self.sent_z.at[0, way],
                    self.arrived.at[self.rank],
                    res=peer,
                )

        self.pass_on(self.rank)

    def hop(self, hop):
        for way in range(2):
            owner, there, onward, peer = self.ends(hop, way)

            @pl.when(there)
            def _():
                wait_for(self.tile(owner), self.arrived.at[owner])

                @pl.when(onward)
                def _():
                    send(
                        self.tile(owner),
                        self.tile(owner),
                        self.sent_z.at[hop, way],
                        self.arrived.at[owner],
                        res=peer,
                    )

                self.pass_on(owner)

    def across(self):
        for d in range(1, self.wide):
            for z in range(self.deep):
                owner = z * self.wide + (self.x + d) % self.wide
                wait_for(self.tile(owner), self.arrived.at[owner])
                if self.forward is not None:
                    self.forward(owner)

    def finish(self):
        for hop in range(self.deep):
            for way in range(2):
                owner, there, onward, _ = self.ends(hop, way)

                @pl.when(jnp.logical_and(there, onward))
                def _():
                    wait_for(self.tile(owner), self.sent_z.at[hop, way])

        for d in range(1, self.wide):
            wait_for(self.tiles(self.deep), self.sent_x)


def fused_kernel(heads, ranks, wide, x_ref, pair_ref, *refs):
    (
        gain_ref,
        probe_ref,
        offset_ref,
        final_ref,
        ff_gain_ref,
        widen_ref,
        shrink_ref,
        opm_gain_ref,
        left_w_ref,
        right_w_ref,
        pair_gain_ref,
        pair_w_ref,
    ), refs = refs[:12], refs[12:]
    (out_ref, right_ref, left_ref), refs = refs[:3], refs[3:]
    (xbuf, pairv, tile_s, tiles, bias, acc, stage, ret, normal, left_v), sems = refs[:10], refs[10:]
    (
        pair_sem,
        x_in,
        x_out,
        ret_in,
        ret_out,
        tile_in,
        tile_z,
        tile_x,
        twin_out,
        twin_in,
        right_in,
        right_z,
        right_x,
        half_out,
        half_in,
        half_own,
        out_sem,
        left_sem,
    ) = sems
    rank = lax.axis_index("res")
    core = lax.axis_index("seq")
    blocks, steps, rows, width = xbuf.shape
    length = blocks * rows
    depth = width // heads
    factor = left_w_ref.shape[0]
    cols = length // 2
    spans = steps // GROUP
    deep = ranks // wide
    per = steps // RETURNS

    barrier = pltpu.get_barrier_semaphore()
    for d in range(1, blocks):
        pl.semaphore_signal(
            barrier, inc=1, device_id={"res": (rank + d) % blocks}, device_id_type=MESH
        )
    pl.semaphore_signal(barrier, inc=1, device_id={"seq": 1 - core}, device_id_type=MESH)
    pl.semaphore_wait(barrier, blocks)

    def send_x(s):
        for d in range(1, blocks):
            to = (rank + d) % blocks
            send(x_ref.at[to * steps + s], xbuf.at[rank, s], x_out.at[0], x_in.at[s], res=to)
        pltpu.make_async_copy(x_ref.at[rank * steps + s], xbuf.at[rank, s], x_in.at[s]).start()

    def send_back(s):
        for d in range(1, blocks):
            to = (rank + d) % blocks
            send(
                xbuf.at[to, s], ret.at[rank * steps + s], ret_out.at[0], ret_in.at[s // per], res=to
            )
        pltpu.make_async_copy(
            xbuf.at[rank, s], ret.at[rank * steps + s], ret_in.at[s // per]
        ).start()

    pair_copy = pltpu.make_async_copy(pair_ref, pairv, pair_sem.at[0])
    pair_copy.start()
    for s in range(2):
        send_x(s)
    pair_copy.wait()

    def tile_rows(i, carry):
        values = pairv[i].astype(jnp.float32)
        normed = layer_normalize(values, pair_gain_ref[...])
        tile = lax.dot_general(
            pair_w_ref[...],
            normed,
            (((1,), (1,)), ((), ())),
            precision=lax.Precision.HIGHEST,
            preferred_element_type=jnp.float32,
        )
        for h in range(heads):
            tile_s[h, pl.ds(i, 1), :] = tile[h : h + 1]
        return carry

    lax.fori_loop(0, rows, tile_rows, 0, unroll=4)
    pack = LANES // rows
    for p in range(heads // pack):
        both = tile_s[p * pack : (p + 1) * pack].reshape(LANES, cols)
        tiles[core, rank, p] = both.T.astype(jnp.bfloat16)

    def to_twin(owner):
        send(
            tiles.at[core, owner], tiles.at[core, owner], twin_out.at[0], twin_in.at[0], seq=1 - core
        )

    spread = Relay(
        rank,
        deep,
        wide,
        lambda o: tiles.at[core, o],
        lambda c: tiles.at[core, pl.ds(0, c)],
        tile_in,
        tile_z,
        tile_x.at[0],
        to_twin,
    )
    send_x(2)
    spread.start()
    for hop in range(1, deep):
        if hop + 2 < AHEAD:
            send_x(hop + 2)
        spread.hop(hop)
    for s in range(min(deep + 2, AHEAD), AHEAD):
        send_x(s)
    spread.across()
    wait_for(tiles.at[1 - core], twin_in.at[0])

    low = lax.broadcasted_iota(jnp.int32, (cols, LANES), 1) < rows

    def fill(step, carry):
        half, p = step // (heads // pack), step % (heads // pack)
        for k in range(blocks // pack):
            even = tiles[half, pack * k, p].astype(jnp.float32) * LOG2E
            odd = tiles[half, pack * k + 1, p].astype(jnp.float32) * LOG2E
            here = (pl.ds(pl.multiple_of(half * cols, cols), cols), slice(k * LANES, (k + 1) * LANES))
            bias[(pack * p,) + here] = jnp.where(low, even, pltpu.roll(odd, rows, 1))
            bias[(pack * p + 1,) + here] = jnp.where(low, pltpu.roll(even, rows, 1), odd)
        return carry

    lax.fori_loop(0, 2 * heads // pack, fill, 0)

    def relay_of(u):
        return Relay(
            rank,
            deep,
            wide,
            lambda o: right_ref.at[:, o, u],
            lambda c: right_ref.at[:, pl.ds(0, c), u],
            right_in.at[u],
            right_z.at[u],
            right_x.at[u],
        )

    def swap_halves(u):
        send(stage.at[u, 1], right_ref.at[core, rank, u], half_out.at[u], half_in.at[u], seq=1 - core)
        pltpu.make_async_copy(stage.at[u, 0], right_ref.at[core, rank, u], half_own.at[u]).start()

    def start_right(u):
        wait_for(right_ref.at[core, rank, u], half_own.at[u])
        wait_for(right_ref.at[1 - core, rank, u], half_in.at[u])
        relay_of(u).start()

    ones = jnp.ones((16, length), jnp.bfloat16)

    def sequence(s, carry):
        wait_for(xbuf.at[:, s], x_in.at[s])

        @pl.when(s + AHEAD < steps)
        def _():
            send_x(s + AHEAD)

        u, place = s // GROUP - 1, s % GROUP

        @pl.when(jnp.logical_and(u >= 0, place == 0))
        def _():
            swap_halves(u)

        @pl.when(s > 0)
        def _():
            send_back(s - 1)

        @pl.when(jnp.logical_and(u >= 0, place == 1))
        def _():
            start_right(u)

        @pl.when(jnp.logical_and(u >= 0, jnp.logical_and(place > 1, place <= deep)))
        def _():
            relay_of(u).hop(place - 1)

        x = xbuf[:, s].astype(jnp.float32).reshape(length, width)
        normed = layer_normalize(x, gain_ref[...]).astype(jnp.bfloat16)
        mapped = dot_t(probe_ref[...], normed)
        q = (mapped[:width] * (depth ** (-0.5) * LOG2E)).astype(jnp.bfloat16)
        k = mapped[width : 2 * width].astype(jnp.bfloat16)
        v = mapped[2 * width : 3 * width].astype(jnp.bfloat16)
        gate = jax.nn.sigmoid(mapped[3 * width :] + offset_ref[...])
        gated = []
        for h in range(heads):
            part = slice(h * depth, (h + 1) * depth)
            scores = dot_f32(k[part], q[part], 0, 0) + bias[h]
            top = jnp.max(scores, axis=0, keepdims=True)
            p = jnp.exp2(scores - top).astype(jnp.bfloat16)
            mixed = dot_f32(jnp.concatenate([v[part], ones], axis=0), p, 1, 0)
            share = mixed[:depth] / mixed[depth : depth + 1]
            gated.append((share * gate[part]).astype(jnp.bfloat16))
        gated = jnp.concatenate(gated, axis=0)
        stream = x + dot_f32(gated, final_ref[...], 0, 0)
        normed = layer_normalize(stream, ff_gain_ref[...]).astype(jnp.bfloat16)
        hidden = jnp.maximum(dot_f32(normed, widen_ref[...], 1, 0), 0.0).astype(jnp.bfloat16)
        stream = stream + dot_f32(hidden, shrink_ref[...], 1, 0)
        updated = stream.astype(jnp.bfloat16)
        xbuf[:, s] = stream.reshape(blocks, rows, width).astype(jnp.bfloat16)
        normed = layer_normalize(updated.astype(jnp.float32), opm_gain_ref[...]).astype(jnp.bfloat16)
        right = dot_t(right_w_ref[...], normed)
        for e in range(factor):
            acc[e, pl.ds(place, 1), :] = right[e : e + 1]

        @pl.when(place == GROUP - 1)
        def _():
            own = pl.ds(pl.multiple_of(core * cols, cols), cols)
            other = pl.ds(pl.multiple_of((1 - core) * cols, cols), cols)
            stage[u + 1, 0] = acc[:, :, own].astype(jnp.bfloat16)
            stage[u + 1, 1] = acc[:, :, other].astype(jnp.bfloat16)

        return carry

    lax.fori_loop(0, steps, sequence, 0)

    last = spans - 1
    swap_halves(last)
    send_back(steps - 1)
    start_right(last)
    for hop in range(1, deep):
        relay_of(last).hop(hop)
    for u in range(spans):
        relay_of(u).across()

    for part in range(RETURNS):
        wait_for(ret.at[pl.ds(0, blocks * per)], ret_in.at[part])

        def normalize(b, carry):
            first = b * steps + part * per
            values = ret[pl.ds(first, per)].astype(jnp.float32).reshape(per * rows, width)
            values = layer_normalize(values, opm_gain_ref[...]).astype(jnp.bfloat16)
            place = pl.multiple_of(first * rows, per * rows)
            for c in range(width // LANES):
                lanes = values[:, c * LANES : (c + 1) * LANES]
                normal[c, pl.ds(place, per * rows), :] = lanes.astype(jnp.float32)
            return carry

        lax.fori_loop(0, blocks, normalize, 0)
    out_copy = pltpu.make_async_copy(ret, out_ref, out_sem.at[0])
    out_copy.start()

    def left_rows(i, carry):
        values = jnp.concatenate(
            [
                normal[c, pl.ds(i, blocks * steps, stride=rows), :].astype(jnp.bfloat16)
                for c in range(width // LANES)
            ],
            axis=1,
        )
        place = pl.multiple_of(i * factor, factor)
        left_v[pl.ds(place, factor), :] = dot_t(left_w_ref[...], values).astype(jnp.bfloat16)
        return carry

    lax.fori_loop(0, rows, left_rows, 0, unroll=8)
    keep = pltpu.make_async_copy(left_v, left_ref.at[core], left_sem.at[0])
    keep.start()
    send(left_v, left_ref.at[core], left_sem.at[1], left_sem.at[2], seq=1 - core)

    wait_for(x_ref.at[pl.ds(0, (blocks - 1) * steps)], x_out.at[0])
    wait_for(ret.at[pl.ds(0, (blocks - 1) * steps)], ret_out.at[0])
    spread.finish()
    wait_for(tiles.at[core], twin_out.at[0])
    for u in range(spans):
        relay_of(u).finish()
        wait_for(stage.at[u, 1], half_out.at[u])
    out_copy.wait()
    keep.wait()
    wait_for(left_v, left_sem.at[1])
    wait_for(left_ref.at[1 - core], left_sem.at[2])


def run_fused(x, pair, weights, heads, ranks, wide):
    sequences, rows, width = x.shape
    steps = sequences // ranks
    length = rows * ranks
    cols = pair.shape[1]
    factor = weights[8].shape[0]
    spans = steps // GROUP
    deep = ranks // wide
    pack = LANES // rows
    any_spec = pl.BlockSpec(memory_space=pl.ANY)
    dma = lambda *shape: pltpu.SemaphoreType.DMA(shape)
    return pl.pallas_call(
        functools.partial(fused_kernel, heads, ranks, wide),
        in_specs=[any_spec] * 2 + [pl.BlockSpec(memory_space=pltpu.VMEM)] * len(weights),
        out_specs=[any_spec] * 3,
        out_shape=[
            jax.ShapeDtypeStruct(a, jnp.bfloat16)
            for a in (
                x.shape,
                (2, ranks, spans, factor, GROUP, cols),
                (2, rows * factor, sequences),
            )
        ],
        scratch_shapes=[
            pltpu.VMEM((ranks, steps, rows, width), jnp.bfloat16),
            pltpu.VMEM(pair.shape, jnp.bfloat16),
            pltpu.VMEM((heads, rows, cols), jnp.float32),
            pltpu.VMEM((2, ranks, heads // pack, cols, LANES), jnp.bfloat16),
            pltpu.VMEM((heads, length, length), jnp.float32),
            pltpu.VMEM((factor, GROUP, length), jnp.float32),
            pltpu.VMEM((spans, 2, factor, GROUP, cols), jnp.bfloat16),
            pltpu.VMEM(x.shape, jnp.bfloat16),
            pltpu.VMEM((width // LANES, sequences * rows, LANES), jnp.float32),
            pltpu.VMEM((rows * factor, sequences), jnp.bfloat16),
            dma(1),
            dma(steps),
            dma(1),
            dma(RETURNS),
            dma(1),
            dma(ranks),
            dma(deep, 2),
            dma(1),
            dma(1),
            dma(1),
            dma(spans, ranks),
            dma(spans, deep, 2),
            dma(spans),
            dma(spans),
            dma(spans),
            dma(spans),
            dma(1),
            dma(3),
        ],
        compiler_params=pltpu.CompilerParams(
            vmem_limit_bytes=FUSED_VMEM, collective_id=0, has_side_effects=True
        ),
        name="fused",
    )(x, pair, *weights)


def pair_kernel(rows, seq_total, left_ref, right_ref, table_ref, pair_ref, out_ref, stack):
    factor, cols = right_ref.shape[3], right_ref.shape[5]
    scale = 1.0 / seq_total
    left = jnp.concatenate([left_ref[0], left_ref[1]], axis=1)
    for e in range(factor):
        right = right_ref[:, :, :, e].reshape(seq_total, cols)
        outer = (dot_f32(left, right, 1, 0) * scale).astype(jnp.bfloat16)
        stack[:, e * factor : (e + 1) * factor, :] = outer.reshape(rows, factor, cols)
    for i in range(rows):
        update = dot_f32(table_ref[...], stack[i], 1, 0)
        out_ref[i] = (pair_ref[i].astype(jnp.float32) + update.T).astype(jnp.bfloat16)


def run_pair(left, right, table, pair):
    _, total_rows, half = left.shape
    _, _, _, factor, _, cols = right.shape
    pair_rows, _, width = pair.shape
    rows = math.gcd(pair_rows, 8)
    once = pl.Buffered(1)
    return pl.pallas_call(
        functools.partial(pair_kernel, rows, 2 * half),
        grid=(pair_rows // rows,),
        in_specs=[
            pl.BlockSpec((2, rows * factor, half), lambda b: (0, b, 0)),
            pl.BlockSpec(right.shape, lambda b: (0,) * 6, pipeline_mode=once),
            pl.BlockSpec(table.shape, lambda b: (0, 0), pipeline_mode=once),
            pl.BlockSpec((rows, cols, width), lambda b: (b, 0, 0)),
        ],
        out_specs=pl.BlockSpec((rows, cols, width), lambda b: (b, 0, 0)),
        out_shape=jax.ShapeDtypeStruct(pair.shape, jnp.bfloat16),
        scratch_shapes=[pltpu.VMEM((rows, factor * factor, cols), jnp.bfloat16)],
        compiler_params=pltpu.CompilerParams(
            dimension_semantics=("arbitrary",), vmem_limit_bytes=VMEM_LIMIT // 2
        ),
        name="product",
    )(left, right, table, pair)


def fits(rows, steps, ranks, heads, seq_axis):
    return (
        seq_axis == 2
        and rows * 2 == LANES
        and heads % 2 == 0
        and ranks % 2 == 0
        and steps % GROUP == 0
        and ranks // 2 < GROUP
        and steps >= AHEAD
        and steps % RETURNS == 0
    )


def fused_on_device(
    aligned_activity,
    pair_state,
    focus_scaling_vector,
    combined_probe_matrix,
    sigmoid_offset_vector,
    focus_final_matrix,
    pair_norm_gain,
    pair_bias_matrix,
    feedforward_scaling_vector,
    feedforward_widen_matrix,
    feedforward_shrink_matrix,
    tensor_scaling_vector,
    twin_operand_matrix,
    tensor_final_matrix,
):
    heads = pair_bias_matrix.shape[1]
    factor = twin_operand_matrix.shape[1] // 2
    twin = twin_operand_matrix.T
    weights = (
        focus_scaling_vector.reshape(1, -1),
        combined_probe_matrix.T,
        sigmoid_offset_vector.reshape(-1, 1),
        focus_final_matrix,
        feedforward_scaling_vector.reshape(1, -1),
        feedforward_widen_matrix,
        feedforward_shrink_matrix,
        tensor_scaling_vector.reshape(1, -1),
        twin[:factor],
        twin[factor:],
        pair_norm_gain.reshape(1, -1),
        pair_bias_matrix.T,
    )
    alignment_output, right, left = run_fused(
        aligned_activity, pair_state, weights, heads, lax.axis_size("res"), 2
    )
    table = tensor_final_matrix.reshape(factor, factor, -1).transpose(2, 1, 0)
    table = table.reshape(table.shape[0], -1)
    return (alignment_output, run_pair(left, right, table, pair_state))


def on_device(aligned_activity, pair_state, *parameters):
    ranks = lax.axis_size("res")
    rows = aligned_activity.shape[1]
    steps = aligned_activity.shape[0] // ranks
    heads = parameters[5].shape[1]
    if fits(rows, steps, ranks, heads, lax.axis_size("seq")):
        return fused_on_device(aligned_activity, pair_state, *parameters)
    return permuted_on_device(aligned_activity, pair_state, *parameters)


def solution(mesh):
    return jax.shard_map(
        on_device,
        mesh=mesh,
        in_specs=(
            P(("grp", "seq"), "res", None),
            P(("grp", "res"), "seq", None),
            P(),
            P(),
            P(),
            P(),
            P(),
            P(),
            P(),
            P(),
            P(),
            P(),
            P(),
            P(),
        ),
        out_specs=(P(("grp", "seq"), "res", None), P(("grp", "res"), "seq", None)),
        check_vma=False,
    )
```

```python
import functools
import math

import jax
import jax.numpy as jnp
from jax import lax
from jax.experimental import pallas as pl
from jax.experimental.pallas import tpu as pltpu
from jax.sharding import PartitionSpec as P

LOG2E = math.log2(math.e)
VMEM_LIMIT = 60 * 1024 * 1024
FUSED_VMEM = 67043328
CHUNKS = 4
GROUPS = 2


def layer_normalize(inputs, scale_gain):
    sample_expectation = jnp.mean(inputs, axis=-1, keepdims=True)
    centered = inputs - sample_expectation
    variance = jnp.mean(centered * centered, axis=-1, keepdims=True)
    return centered * lax.rsqrt(variance + 1e-05) * scale_gain


def dot_f32(a, b, ca, cb):
    return lax.dot_general(a, b, (((ca,), (cb,)), ((), ())), preferred_element_type=jnp.float32)


def sequence_kernel(
    heads,
    pack,
    blocks,
    *refs,
):
    rank_ref, refs = refs[0], refs[1:]
    x_refs, refs = refs[:blocks], refs[blocks:]
    weight_refs, refs = refs[:11], refs[11:]
    out_refs, (right_ref, gathered, left_acc, right_acc) = refs[:blocks], refs[blocks:]
    (
        bias_ref,
        gain_ref,
        probe_ref,
        offset_ref,
        final_ref,
        ff_gain_ref,
        widen_ref,
        shrink_ref,
        opm_gain_ref,
        left_w_ref,
        right_w_ref,
    ) = weight_refs
    rank = rank_ref[0]
    step = pl.program_id(0)
    steps = right_ref.shape[2]
    _, rows, width = x_refs[0].shape
    length = blocks * rows
    depth = width // heads
    for d in range(blocks):
        gathered[lax.rem(rank + blocks - d, blocks)] = x_refs[d][0]
    x = gathered[...].astype(jnp.float32).reshape(length, width)
    normed = layer_normalize(x, gain_ref[...]).astype(jnp.bfloat16)
    mapped = dot_f32(probe_ref[...], normed, 1, 1)
    q = (mapped[:width] * (depth ** (-0.5) * LOG2E)).astype(jnp.bfloat16)
    k = mapped[width : 2 * width].astype(jnp.bfloat16)
    v = mapped[2 * width : 3 * width].astype(jnp.bfloat16)
    gate = jax.nn.sigmoid(mapped[3 * width :] + offset_ref[...])
    def due(s):
        early = steps - AHEAD
        slow = early * SLOW // 10
        return jnp.where(s <= early, s * SLOW // 10, slow + s - early)

    def send_back_upto(first, end):
        def one(s, carry):
            send_back(s)
            return carry

        lax.fori_loop(first, end, one, 0)

    ones = jnp.ones((16, length), jnp.bfloat16)
    gated = []
    for h in range(heads):
        part = slice(h * depth, (h + 1) * depth)
        scores = dot_f32(k[part], q[part], 0, 0) + bias_ref[h]
        top = jnp.max(scores, axis=0, keepdims=True)
        p = jnp.exp2(scores - top).astype(jnp.bfloat16)
        mixed = dot_f32(jnp.concatenate([v[part], ones], axis=0), p, 1, 0)
        share = mixed[:depth] / mixed[depth : depth + 1]
        gated.append((share * gate[part]).astype(jnp.bfloat16))
    gated = jnp.concatenate(gated, axis=0)
    stream = x + dot_f32(gated, final_ref[...], 0, 0)
    normed = layer_normalize(stream, ff_gain_ref[...]).astype(jnp.bfloat16)
    hidden = jnp.maximum(dot_f32(normed, widen_ref[...], 1, 0), 0.0).astype(jnp.bfloat16)
    stream = stream + dot_f32(hidden, shrink_ref[...], 1, 0)
    updated = stream.astype(jnp.bfloat16)
    gathered[...] = stream.reshape(blocks, rows, width).astype(jnp.bfloat16)
    for d in range(blocks):
        out_refs[d][step] = gathered[lax.rem(rank + d, blocks)]
    normed = layer_normalize(updated.astype(jnp.float32), opm_gain_ref[...]).astype(jnp.bfloat16)
    slot = lax.rem(step, pack)
    left = dot_f32(normed, left_w_ref[slot], 1, 0).reshape(left_acc.shape)

    @pl.when(slot == 0)
    def _():
        left_acc[...] = left

    @pl.when(slot != 0)
    def _():
        left_acc[...] = left_acc[...] + left

    factor = right_w_ref.shape[0]
    right = dot_f32(right_w_ref[...], normed, 1, 1)
    for e in range(factor):
        right_acc[e, pl.ds(step, 1), :] = right[e : e + 1]

    @pl.when(step == steps - 1)
    def _():
        lanes = left_acc.shape[2]
        cols = right_ref.shape[3]
        for part in range(right_ref.shape[0]):
            right_ref[part] = right_acc[:, :, part * cols : (part + 1) * cols].astype(jnp.bfloat16)
        for d in range(blocks):
            if lanes < width:
                out_refs[d][steps] = jnp.zeros((rows, width), jnp.bfloat16)
            out_refs[d][steps, :, :lanes] = left_acc[lax.rem(rank + d, blocks)].astype(jnp.bfloat16)


def run_sequences(rank, xs, bias, weights, heads, pack, halves):
    blocks = len(xs)
    steps, rows, width = xs[0].shape
    length = blocks * rows
    factor = weights[-1].shape[0]
    cols = length // halves
    whole = lambda a: pl.BlockSpec(
        a.shape, lambda s, n=a.ndim: (0,) * n, pipeline_mode=pl.Buffered(1)
    )
    kept = lambda shape: pl.BlockSpec(shape, lambda s, n=len(shape): (0,) * n)
    lanes = pack * factor
    hidden = weights[5].shape[1]
    flops = 2 * length * width * (5 * width + 2 * hidden + 128) + 4 * length * length * width
    shapes = [(steps + 1, rows, width)] * blocks + [(halves, factor, steps, cols)]
    return pl.pallas_call(
        functools.partial(sequence_kernel, heads, pack, blocks),
        grid=(steps,),
        in_specs=[pl.BlockSpec(memory_space=pltpu.SMEM)]
        + [pl.BlockSpec((1, rows, width), lambda s: (s, 0, 0)) for _ in xs]
        + [whole(a) for a in (bias,) + weights],
        out_specs=[kept(a) for a in shapes],
        out_shape=[jax.ShapeDtypeStruct(a, jnp.bfloat16) for a in shapes],
        scratch_shapes=[
            pltpu.VMEM((blocks, rows, width), jnp.bfloat16),
            pltpu.VMEM((blocks, rows, lanes), jnp.float32),
            pltpu.VMEM((factor, steps, length), jnp.float32),
        ],
        compiler_params=pltpu.CompilerParams(
            dimension_semantics=("arbitrary",), vmem_limit_bytes=VMEM_LIMIT
        ),
        cost_estimate=pl.CostEstimate(
            flops=steps * flops * 3,
            bytes_accessed=bias.size * 4 + 4 * length * width * steps,
            transcendentals=steps * heads * length * length,
        ),
        name="sequences",
    )(rank, *xs, bias, *weights)


def deal_kernel(chunks, rank_ref, x_ref, *out_refs):
    blocks = x_ref.shape[0]
    part = x_ref.shape[1] // chunks
    for c in range(chunks):
        for d in range(blocks):
            source = lax.rem(rank_ref[0] + d, blocks)
            out_refs[c * blocks + d][...] = x_ref[source, c * part : (c + 1) * part]


def collect_kernel(chunks, rank_ref, *refs):
    in_refs, (out_ref, left_ref) = refs[:-2], refs[-2:]
    blocks = out_ref.shape[0]
    part = out_ref.shape[1] // chunks
    lanes = left_ref.shape[3]
    for c in range(chunks):
        for d in range(blocks):
            target = lax.rem(rank_ref[0] + blocks - d, blocks)
            y_ref = in_refs[c * blocks + d]
            out_ref[target, c * part : (c + 1) * part] = y_ref[:part]
            left_ref[target, c] = y_ref[part, :, :lanes]


def vmem_call(kernel, shapes, rank, arrays, name):
    return pl.pallas_call(
        kernel,
        in_specs=[pl.BlockSpec(memory_space=pltpu.SMEM)]
        + [pl.BlockSpec(memory_space=pltpu.VMEM)] * len(arrays),
        out_specs=[pl.BlockSpec(memory_space=pltpu.VMEM)] * len(shapes),
        out_shape=[jax.ShapeDtypeStruct(a, jnp.bfloat16) for a in shapes],
        compiler_params=pltpu.CompilerParams(vmem_limit_bytes=VMEM_LIMIT // 2),
        cost_estimate=pl.CostEstimate(
            flops=0, bytes_accessed=4 * sum(a.size for a in arrays), transcendentals=0
        ),
        name=name,
    )(rank, *arrays)


def shift_all(arrays):
    size = len(arrays)
    return [arrays[0]] + [
        lax.ppermute(arrays[d], "res", [(r, (r + d) % size) for r in range(size)])
        for d in range(1, size)
    ]


def product_kernel(rows, seq_total, left_ref, *refs):
    right_refs, (table_ref, pair_ref, out_ref, stack) = refs[:-4], refs[-4:]
    groups, factor, part, cols = right_refs[0].shape
    scale = 1.0 / seq_total
    left = left_ref[...]
    for e in range(factor):
        right = jnp.concatenate(
            [ref[:, e].reshape(groups * part, cols) for ref in right_refs], axis=0
        )
        outer = (dot_f32(left, right, 1, 0) * scale).astype(jnp.bfloat16)
        stack[:, e * factor : (e + 1) * factor, :] = outer.reshape(rows, factor, cols)
    for i in range(rows):
        update = dot_f32(table_ref[...], stack[i], 1, 0)
        out_ref[i] = (pair_ref[i].astype(jnp.float32) + update.T).astype(jnp.bfloat16)


def run_product(left, rights, table, pair):
    total_rows, seq_total = left.shape
    _, factor, _, cols = rights[0].shape
    pair_rows = pair.shape[0]
    rows = math.gcd(pair_rows, 8)
    width = pair.shape[2]
    return pl.pallas_call(
        functools.partial(product_kernel, rows, seq_total),
        grid=(pair_rows // rows,),
        in_specs=[
            pl.BlockSpec((rows * factor, seq_total), lambda b: (b, 0)),
            *[
                pl.BlockSpec(a.shape, lambda b: (0, 0, 0, 0), pipeline_mode=pl.Buffered(1))
                for a in rights
            ],
            pl.BlockSpec(table.shape, lambda b: (0, 0), pipeline_mode=pl.Buffered(1)),
            pl.BlockSpec((rows, cols, width), lambda b: (b, 0, 0)),
        ],
        out_specs=pl.BlockSpec((rows, cols, width), lambda b: (b, 0, 0)),
        out_shape=jax.ShapeDtypeStruct(pair.shape, jnp.bfloat16),
        scratch_shapes=[pltpu.VMEM((rows, factor * factor, cols), jnp.bfloat16)],
        compiler_params=pltpu.CompilerParams(
            dimension_semantics=("arbitrary",), vmem_limit_bytes=VMEM_LIMIT
        ),
        cost_estimate=pl.CostEstimate(
            flops=4 * total_rows * cols * factor * (seq_total + width),
            bytes_accessed=2 * (left.size * (1 + cols * factor // total_rows) + left.size + 2 * pair.size),
            transcendentals=0,
        ),
        name="product",
    )(left, *rights, table, pair)


def permuted_on_device(
    aligned_activity,
    pair_state,
    focus_scaling_vector,
    combined_probe_matrix,
    sigmoid_offset_vector,
    focus_final_matrix,
    pair_norm_gain,
    pair_bias_matrix,
    feedforward_scaling_vector,
    feedforward_widen_matrix,
    feedforward_shrink_matrix,
    tensor_scaling_vector,
    twin_operand_matrix,
    tensor_final_matrix,
):
    width = aligned_activity.shape[2]
    heads = pair_bias_matrix.shape[1]
    factor = twin_operand_matrix.shape[1] // 2
    res_axis = lax.axis_size("res")
    seq_axis = lax.axis_size("seq")
    rows = aligned_activity.shape[1]
    seq_count = aligned_activity.shape[0] // res_axis
    length = rows * res_axis
    col_block = pair_state.shape[1]
    chunks = math.gcd(CHUNKS, seq_count)
    per_chunk = seq_count // chunks
    pack = per_chunk

    groups = math.gcd(GROUPS, chunks) if seq_count % (8 * GROUPS) == 0 else 1
    rank = lax.axis_index("res").astype(jnp.int32).reshape(1)
    pieces = aligned_activity.reshape(res_axis, seq_count, rows, width)
    dealt = vmem_call(
        functools.partial(deal_kernel, chunks),
        [(per_chunk, rows, width)] * (chunks * res_axis),
        rank,
        [pieces],
        "deal",
    )
    arrived = [shift_all(dealt[c * res_axis : (c + 1) * res_axis]) for c in range(chunks)]

    pair_norm = layer_normalize(pair_state.astype(jnp.float32), pair_norm_gain)
    bias_tile = jnp.einsum(
        "ijc,ch->hij", pair_norm, pair_bias_matrix, precision=lax.Precision.HIGHEST
    ).astype(jnp.bfloat16)
    bias_rows = lax.all_gather(bias_tile, "res", axis=1, tiled=True)
    bias_all = lax.all_gather(bias_rows, "seq", axis=0)
    bias = bias_all.transpose(1, 0, 3, 2).reshape(heads, length, length)
    bias = bias.astype(jnp.float32) * LOG2E

    left_w = twin_operand_matrix[:, :factor]
    left_w = jnp.stack(
        [jnp.pad(left_w, ((0, 0), (t * factor, (pack - 1 - t) * factor))) for t in range(pack)]
    )
    weights = (
        focus_scaling_vector.reshape(1, -1),
        combined_probe_matrix.T,
        sigmoid_offset_vector.reshape(-1, 1),
        focus_final_matrix,
        feedforward_scaling_vector.reshape(1, -1),
        feedforward_widen_matrix,
        feedforward_shrink_matrix,
        tensor_scaling_vector.reshape(1, -1),
        left_w,
        twin_operand_matrix[:, factor:].T,
    )
    returned, rights, pending = [], [], []
    for c in range(chunks):
        *updated, right = run_sequences(rank, arrived[c], bias, weights, heads, pack, seq_axis)
        returned += shift_all(updated)
        pending.append(right)
        if len(pending) == chunks // groups:
            right = jnp.concatenate(pending, axis=2)
            right = lax.all_to_all(right, "seq", split_axis=0, concat_axis=0, tiled=True)
            rights.append(lax.all_gather(right, "res", axis=0, tiled=True))
            pending = []
    if (seq_count // groups) % 8 != 0:
        rights = [r.transpose(1, 0, 2, 3).reshape(1, factor, -1, col_block) for r in rights]
    alignment_output, left = vmem_call(
        functools.partial(collect_kernel, chunks),
        [pieces.shape, (res_axis, chunks, rows, pack * factor)],
        rank,
        returned,
        "collect",
    )
    alignment_output = alignment_output.reshape(aligned_activity.shape)
    left = lax.all_gather(left, "seq", axis=0)
    left = left.reshape(seq_axis, res_axis, groups, chunks // groups, rows, pack, factor)
    left = left.transpose(4, 6, 2, 1, 0, 3, 5).reshape(rows * factor, -1)

    table = tensor_final_matrix.reshape(factor, factor, -1).transpose(2, 1, 0)
    table = table.reshape(table.shape[0], -1)
    pair_output = run_product(left, rights, table, pair_state)
    return (alignment_output, pair_output)


MESH = pl.DeviceIdType.MESH
GROUP = 8
AHEAD = 6
FIRST = 3
SLOW = 3
LANES = 128


def dot_t(a, b):
    return dot_f32(a, b, 1, 1)


def wait_for(ref, sem):
    pltpu.make_async_copy(ref, ref, sem).wait()


def send(src, dst, sent, arrived, **peer):
    pltpu.make_async_remote_copy(
        src_ref=src,
        dst_ref=dst,
        send_sem=sent,
        recv_sem=arrived,
        device_id=peer,
        device_id_type=MESH,
    ).start()


class Relay:
    def __init__(self, rank, deep, wide, tile, tiles, arrived, sent_z, sent_x, forward=None):
        self.rank, self.deep, self.wide = rank, deep, wide
        self.z, self.x = rank // wide, rank % wide
        self.tile, self.tiles, self.arrived = tile, tiles, arrived
        self.sent_z, self.sent_x, self.forward = sent_z, sent_x, forward

    def pass_on(self, owner):
        for d in range(1, self.wide):
            peer = self.z * self.wide + (self.x + d) % self.wide
            send(self.tile(owner), self.tile(owner), self.sent_x, self.arrived.at[owner], res=peer)
        if self.forward is not None:
            self.forward(owner)

    def ends(self, hop, way):
        z = self.z - hop if way == 0 else self.z + hop
        there = z >= 0 if way == 0 else z < self.deep
        onward = self.z + 1 < self.deep if way == 0 else self.z >= 1
        peer = self.rank + self.wide if way == 0 else self.rank - self.wide
        return z * self.wide + self.x, there, onward, peer

    def start(self):
        for way in range(2):
            owner, _, onward, peer = self.ends(0, way)

            @pl.when(onward)
            def _():
                send(
                    self.tile(self.rank),
                    self.tile(self.rank),
                    self.sent_z.at[0, way],
                    self.arrived.at[self.rank],
                    res=peer,
                )

        self.pass_on(self.rank)

    def hop(self, hop):
        for way in range(2):
            owner, there, onward, peer = self.ends(hop, way)

            @pl.when(there)
            def _():
                wait_for(self.tile(owner), self.arrived.at[owner])

                @pl.when(onward)
                def _():
                    send(
                        self.tile(owner),
                        self.tile(owner),
                        self.sent_z.at[hop, way],
                        self.arrived.at[owner],
                        res=peer,
                    )

                self.pass_on(owner)

    def across(self):
        for d in range(1, self.wide):
            for z in range(self.deep):
                owner = z * self.wide + (self.x + d) % self.wide
                wait_for(self.tile(owner), self.arrived.at[owner])
                if self.forward is not None:
                    self.forward(owner)

    def finish(self):
        for hop in range(self.deep):
            for way in range(2):
                owner, there, onward, _ = self.ends(hop, way)

                @pl.when(jnp.logical_and(there, onward))
                def _():
                    wait_for(self.tile(owner), self.sent_z.at[hop, way])

        for d in range(1, self.wide):
            wait_for(self.tiles(self.deep), self.sent_x)


def fused_kernel(heads, ranks, wide, x_ref, pair_ref, *refs):
    given, refs = refs[:12], refs[12:]
    (out_ref, pair_out_ref), refs = refs[:2], refs[2:]
    held, refs = refs[:12], refs[12:]
    (
        gain_ref,
        probe_rows,
        offset_row,
        final_ref,
        ff_gain_ref,
        widen_ref,
        shrink_ref,
        opm_gain_ref,
        twin_ref,
        pair_gain_ref,
        pair_w_ref,
        table_rows,
    ) = held
    (
        xbuf,
        pairv,
        tile_s,
        tiles,
        bias,
        acc,
        left_acc,
        stage,
        right_v,
        left_out,
        left_in,
        left_s,
        left_v,
        stack,
        probe_ref,
        offset_ref,
        table_s,
        table_ref,
    ), sems = refs[:18], refs[18:]
    (
        pair_sem,
        held_sem,
        x_in,
        x_out,
        ret_in,
        ret_out,
        tile_in,
        tile_z,
        tile_x,
        twin_out,
        twin_in,
        right_in,
        right_z,
        right_x,
        half_out,
        half_in,
        half_own,
        left_sem,
    ) = sems
    rank = lax.axis_index("res")
    core = lax.axis_index("seq")
    blocks, steps, rows, width = xbuf.shape
    length = blocks * rows
    depth = width // heads
    factor = twin_ref.shape[0] // 2
    cols = length // 2
    spans = steps // GROUP
    deep = ranks // wide

    barrier = pltpu.get_barrier_semaphore()
    for d in range(1, blocks):
        pl.semaphore_signal(
            barrier, inc=1, device_id={"res": (rank + d) % blocks}, device_id_type=MESH
        )
    pl.semaphore_signal(barrier, inc=1, device_id={"seq": 1 - core}, device_id_type=MESH)
    pl.semaphore_wait(barrier, blocks)

    def send_x(s):
        for d in range(1, blocks):
            to = (rank + d) % blocks
            send(x_ref.at[to * steps + s], xbuf.at[rank, s], x_out.at[0], x_in.at[s], res=to)
        pltpu.make_async_copy(x_ref.at[rank * steps + s], xbuf.at[rank, s], x_in.at[s]).start()

    def send_back(s):
        for d in range(1, blocks):
            to = (rank + d) % blocks
            send(xbuf.at[to, s], out_ref.at[rank * steps + s], ret_out.at[0], ret_in.at[0], res=to)
        pltpu.make_async_copy(xbuf.at[rank, s], out_ref.at[rank * steps + s], ret_in.at[0]).start()

    pair_copy = pltpu.make_async_copy(pair_ref, pairv, pair_sem.at[0])
    pair_copy.start()
    for s in range(FIRST):
        send_x(s)
    copies = [
        pltpu.make_async_copy(given[i], held[i], held_sem.at[i]) for i in range(len(given))
    ]
    for copy in copies:
        copy.start()
    for copy in copies:
        copy.wait()
    pair_copy.wait()

    def tile_rows(i, carry):
        values = pairv[i].astype(jnp.float32)
        normed = layer_normalize(values, pair_gain_ref[...])
        tile = lax.dot_general(
            pair_w_ref[...],
            normed,
            (((1,), (1,)), ((), ())),
            precision=lax.Precision.HIGHEST,
            preferred_element_type=jnp.float32,
        )
        for h in range(heads):
            tile_s[h, pl.ds(i, 1), :] = tile[h : h + 1]
        return carry

    lax.fori_loop(0, rows, tile_rows, 0, unroll=4)
    pack = LANES // rows
    for p in range(heads // pack):
        both = tile_s[p * pack : (p + 1) * pack].reshape(LANES, cols)
        tiles[core, rank, p] = both.T.astype(jnp.bfloat16)

    def to_twin(owner):
        send(
            tiles.at[core, owner], tiles.at[core, owner], twin_out.at[0], twin_in.at[0], seq=1 - core
        )

    spread = Relay(
        rank,
        deep,
        wide,
        lambda o: tiles.at[core, o],
        lambda c: tiles.at[core, pl.ds(0, c)],
        tile_in,
        tile_z,
        tile_x.at[0],
        to_twin,
    )

    def prepare():
        for c in range(0, probe_rows.shape[1], width):
            columns = probe_rows[:, c : c + width].astype(jnp.float32)
            probe_ref[c : c + width] = columns.T.astype(jnp.bfloat16)
        offset_ref[...] = jnp.broadcast_to(offset_row[...], (LANES, width)).T
        table_s[...] = table_rows[...].astype(jnp.float32)
        few = LANES // factor
        for e in range(0, factor, few):
            lines = [table_s[pl.ds(e + i, factor, stride=factor), :] for i in range(few)]
            lines = jnp.concatenate(lines, axis=0)
            table_ref[:, e * factor : (e + few) * factor] = lines.T.astype(jnp.bfloat16)

    spread.start()
    send_x(FIRST)
    prepare()
    for hop in range(1, deep):
        spread.hop(hop)
        if FIRST + hop < AHEAD:
            send_x(FIRST + hop)
    for s in range(min(FIRST + deep, AHEAD), AHEAD):
        send_x(s)
    spread.across()
    wait_for(tiles.at[1 - core], twin_in.at[0])

    low = lax.broadcasted_iota(jnp.int32, (cols, LANES), 1) < rows

    def fill(step, carry):
        half, p = step // (heads // pack), step % (heads // pack)
        for k in range(blocks // pack):
            even = tiles[half, pack * k, p].astype(jnp.float32) * LOG2E
            odd = tiles[half, pack * k + 1, p].astype(jnp.float32) * LOG2E
            here = (pl.ds(pl.multiple_of(half * cols, cols), cols), slice(k * LANES, (k + 1) * LANES))
            bias[(pack * p,) + here] = jnp.where(low, even, pltpu.roll(odd, rows, 1))
            bias[(pack * p + 1,) + here] = jnp.where(low, pltpu.roll(even, rows, 1), odd)
        return carry

    lax.fori_loop(0, 2 * heads // pack, fill, 0)

    def relay_of(u):
        return Relay(
            rank,
            deep,
            wide,
            lambda o: right_v.at[:, u, o],
            lambda c: right_v.at[:, u, pl.ds(0, c)],
            right_in.at[u],
            right_z.at[u],
            right_x.at[u],
        )

    def swap_halves(u):
        send(stage.at[u, 1], right_v.at[core, u, rank], half_out.at[u], half_in.at[u], seq=1 - core)
        pltpu.make_async_copy(stage.at[u, 0], right_v.at[core, u, rank], half_own.at[u]).start()

    def start_right(u):
        wait_for(right_v.at[core, u, rank], half_own.at[u])
        wait_for(right_v.at[1 - core, u, rank], half_in.at[u])
        relay_of(u).start()

    def due(s):
        early = steps - AHEAD
        slow = early * SLOW // 10
        return jnp.where(s <= early, s * SLOW // 10, slow + s - early)

    def send_back_upto(first, end):
        def one(s, carry):
            send_back(s)
            return carry

        lax.fori_loop(first, end, one, 0)

    ones = jnp.ones((16, length), jnp.bfloat16)

    def sequence(s, carry):
        wait_for(xbuf.at[:, s], x_in.at[s])

        @pl.when(s + AHEAD < steps)
        def _():
            send_x(s + AHEAD)

        u, place = s // GROUP - 1, s % GROUP

        @pl.when(jnp.logical_and(u >= 0, place == 0))
        def _():
            swap_halves(u)

        send_back_upto(due(s), due(s + 1))

        @pl.when(jnp.logical_and(u >= 0, place == 1))
        def _():
            start_right(u)

        @pl.when(jnp.logical_and(u >= 0, jnp.logical_and(place > 1, place <= deep)))
        def _():
            relay_of(u).hop(place - 1)

        x = xbuf[:, s].astype(jnp.float32).reshape(length, width)
        normed = layer_normalize(x, gain_ref[...]).astype(jnp.bfloat16)
        mapped = dot_t(probe_ref[...], normed)
        q = (mapped[:width] * (depth ** (-0.5) * LOG2E)).astype(jnp.bfloat16)
        k = mapped[width : 2 * width].astype(jnp.bfloat16)
        v = mapped[2 * width : 3 * width].astype(jnp.bfloat16)
        gate = jax.nn.sigmoid(mapped[3 * width :] + offset_ref[:, :1])
        gated = []
        for h in range(heads):
            part = slice(h * depth, (h + 1) * depth)
            scores = dot_f32(k[part], q[part], 0, 0) + bias[h]
            top = jnp.max(scores, axis=0, keepdims=True)
            p = jnp.exp2(scores - top).astype(jnp.bfloat16)
            mixed = dot_f32(jnp.concatenate([v[part], ones], axis=0), p, 1, 0)
            share = mixed[:depth] / mixed[depth : depth + 1]
            gated.append((share * gate[part]).astype(jnp.bfloat16))
        gated = jnp.concatenate(gated, axis=0)
        stream = x + dot_f32(gated, final_ref[...], 0, 0)
        normed = layer_normalize(stream, ff_gain_ref[...]).astype(jnp.bfloat16)
        hidden = jnp.maximum(dot_f32(normed, widen_ref[...], 1, 0), 0.0).astype(jnp.bfloat16)
        stream = stream + dot_f32(hidden, shrink_ref[...], 1, 0)
        updated = stream.astype(jnp.bfloat16)
        xbuf[:, s] = stream.reshape(blocks, rows, width).astype(jnp.bfloat16)
        normed = layer_normalize(updated.astype(jnp.float32), opm_gain_ref[...]).astype(jnp.bfloat16)
        factors = dot_t(twin_ref[...], normed)
        for e in range(factor):
            left_acc[e, pl.ds(s, 1), :] = factors[e : e + 1]
            acc[e, pl.ds(place, 1), :] = factors[factor + e : factor + e + 1]

        @pl.when(place == GROUP - 1)
        def _():
            own = pl.ds(pl.multiple_of(core * cols, cols), cols)
            other = pl.ds(pl.multiple_of((1 - core) * cols, cols), cols)
            stage[u + 1, 0] = acc[:, :, own].astype(jnp.bfloat16)
            stage[u + 1, 1] = acc[:, :, other].astype(jnp.bfloat16)

        return carry

    lax.fori_loop(0, steps, sequence, 0)

    last = spans - 1
    sent = due(steps)
    swap_halves(last)
    near = lax.broadcasted_iota(jnp.int32, (factor, GROUP, LANES), 2) < rows
    for m in range(blocks // 2):
        lanes = slice(m * LANES, (m + 1) * LANES)
        one, two = left_acc[:, :GROUP, lanes], left_acc[:, GROUP:, lanes]
        left_out[2 * m] = jnp.where(near, one, pltpu.roll(two, rows, 2)).astype(jnp.bfloat16)
        left_out[2 * m + 1] = jnp.where(near, pltpu.roll(one, rows, 2), two).astype(jnp.bfloat16)
    start_right(last)
    for d in range(1, blocks):
        to = (rank + d) % blocks
        send(left_out.at[to], left_in.at[rank], left_sem.at[0], left_sem.at[1], res=to)
    pltpu.make_async_copy(left_out.at[rank], left_in.at[rank], left_sem.at[1]).start()
    for hop in range(1, deep):
        relay_of(last).hop(hop)
        send_back(sent + hop - 1)
    send_back_upto(sent + deep - 1, steps)

    wait_for(left_in, left_sem.at[1])
    for c in range(factor):
        values = left_in[:, c].astype(jnp.float32).reshape(blocks * GROUP, LANES).T
        values = jnp.concatenate([values[:rows], values[rows:]], axis=1)
        left_s[pl.ds(c, rows, stride=factor), :] = values
    left_v[core] = left_s[...].astype(jnp.bfloat16)
    send(left_v.at[core], left_v.at[core], left_sem.at[2], left_sem.at[3], seq=1 - core)
    for u in range(spans):
        relay_of(u).across()
    wait_for(left_v.at[1 - core], left_sem.at[3])

    some = stack.shape[0]
    scale = 1.0 / (2 * blocks * steps)

    def pair_block(b, carry):
        place = pl.ds(pl.multiple_of(b * some * factor, some * factor), some * factor)
        left = jnp.concatenate([left_v[0, place, :], left_v[1, place, :]], axis=1)
        for e in range(factor):
            right = right_v[:, :, :, e].reshape(2 * blocks * steps, cols)
            outer = (dot_f32(left, right, 1, 0) * scale).astype(jnp.bfloat16)
            stack[:, e * factor : (e + 1) * factor, :] = outer.reshape(some, factor, cols)
        for i in range(some):
            update = dot_f32(table_ref[...], stack[i], 1, 0)
            at = b * some + i
            pairv[at] = (pairv[at].astype(jnp.float32) + update.T).astype(jnp.bfloat16)
        these = pl.ds(b * some, some)
        pltpu.make_async_copy(pairv.at[these], pair_out_ref.at[these], pair_sem.at[1]).start()
        return carry

    lax.fori_loop(0, rows // some, pair_block, 0)

    wait_for(x_ref.at[pl.ds(0, (blocks - 1) * steps)], x_out.at[0])
    wait_for(out_ref.at[pl.ds(0, (blocks - 1) * steps)], ret_out.at[0])
    spread.finish()
    wait_for(tiles.at[core], twin_out.at[0])
    for u in range(spans):
        relay_of(u).finish()
        wait_for(stage.at[u, 1], half_out.at[u])
    wait_for(left_out.at[pl.ds(0, blocks - 1)], left_sem.at[0])
    wait_for(left_v.at[core], left_sem.at[2])
    wait_for(out_ref, ret_in.at[0])
    wait_for(pairv, pair_sem.at[1])


def run_fused(x, pair, weights, heads, ranks, wide):
    sequences, rows, width = x.shape
    steps = sequences // ranks
    length = rows * ranks
    cols = pair.shape[1]
    factor = weights[8].shape[0] // 2
    spans = steps // GROUP
    deep = ranks // wide
    pack = LANES // rows
    table = weights[11].shape
    any_spec = pl.BlockSpec(memory_space=pl.ANY)
    dma = lambda *shape: pltpu.SemaphoreType.DMA(shape)
    half = lambda *shape: pltpu.VMEM(shape, jnp.bfloat16)
    full = lambda *shape: pltpu.VMEM(shape, jnp.float32)
    return pl.pallas_call(
        functools.partial(fused_kernel, heads, ranks, wide),
        in_specs=[any_spec] * (2 + len(weights)),
        out_specs=[any_spec] * 2,
        out_shape=[jax.ShapeDtypeStruct(a, jnp.bfloat16) for a in (x.shape, pair.shape)],
        scratch_shapes=[pltpu.VMEM(a.shape, a.dtype) for a in weights]
        + [
            half(ranks, steps, rows, width),
            half(*pair.shape),
            full(heads, rows, cols),
            half(2, ranks, heads // pack, cols, LANES),
            full(heads, length, length),
            full(factor, GROUP, length),
            full(factor, steps, length),
            half(spans, 2, factor, GROUP, cols),
            half(2, spans, ranks, factor, GROUP, cols),
            half(ranks, factor, GROUP, LANES),
            half(ranks, factor, GROUP, LANES),
            full(rows * factor, LANES),
            half(2, rows * factor, LANES),
            half(math.gcd(rows, 8), factor * factor, cols),
            half(4 * width, width),
            full(width, LANES),
            full(*table),
            half(table[1], table[0]),
            dma(2),
            dma(len(weights)),
            dma(steps),
            dma(1),
            dma(1),
            dma(1),
            dma(ranks),
            dma(deep, 2),
            dma(1),
            dma(1),
            dma(1),
            dma(spans, ranks),
            dma(spans, deep, 2),
            dma(spans),
            dma(spans),
            dma(spans),
            dma(spans),
            dma(4),
        ],
        compiler_params=pltpu.CompilerParams(
            vmem_limit_bytes=FUSED_VMEM, collective_id=0, has_side_effects=True
        ),
        name="fused",
    )(x, pair, *weights)


def fits(rows, steps, ranks, heads, seq_axis):
    return (
        seq_axis == 2
        and rows * 2 == LANES
        and heads % 2 == 0
        and ranks % 2 == 0
        and steps == 2 * GROUP
        and ranks // 2 < GROUP
        and steps >= AHEAD
    )


def fused_on_device(
    aligned_activity,
    pair_state,
    focus_scaling_vector,
    combined_probe_matrix,
    sigmoid_offset_vector,
    focus_final_matrix,
    pair_norm_gain,
    pair_bias_matrix,
    feedforward_scaling_vector,
    feedforward_widen_matrix,
    feedforward_shrink_matrix,
    tensor_scaling_vector,
    twin_operand_matrix,
    tensor_final_matrix,
):
    heads = pair_bias_matrix.shape[1]
    weights = (
        focus_scaling_vector.reshape(1, -1),
        combined_probe_matrix,
        sigmoid_offset_vector.reshape(1, -1),
        focus_final_matrix,
        feedforward_scaling_vector.reshape(1, -1),
        feedforward_widen_matrix,
        feedforward_shrink_matrix,
        tensor_scaling_vector.reshape(1, -1),
        twin_operand_matrix.T,
        pair_norm_gain.reshape(1, -1),
        pair_bias_matrix.T,
        tensor_final_matrix,
    )
    return tuple(
        run_fused(aligned_activity, pair_state, weights, heads, lax.axis_size("res"), 2)
    )


def on_device(aligned_activity, pair_state, *parameters):
    ranks = lax.axis_size("res")
    rows = aligned_activity.shape[1]
    steps = aligned_activity.shape[0] // ranks
    heads = parameters[5].shape[1]
    if fits(rows, steps, ranks, heads, lax.axis_size("seq")):
        return fused_on_device(aligned_activity, pair_state, *parameters)
    return permuted_on_device(aligned_activity, pair_state, *parameters)


def solution(mesh):
    return jax.shard_map(
        on_device,
        mesh=mesh,
        in_specs=(
            P(("grp", "seq"), "res", None),
            P(("grp", "res"), "seq", None),
            P(),
            P(),
            P(),
            P(),
            P(),
            P(),
            P(),
            P(),
            P(),
            P(),
            P(),
            P(),
        ),
        out_specs=(P(("grp", "seq"), "res", None), P(("grp", "res"), "seq", None)),
        check_vma=False,
    )
```

```python
import functools
import math

import jax
import jax.numpy as jnp
from jax import lax
from jax.experimental import pallas as pl
from jax.experimental.pallas import tpu as pltpu
from jax.sharding import PartitionSpec as P

LOG2E = math.log2(math.e)
VMEM_LIMIT = 60 * 1024 * 1024
FUSED_VMEM = 54 * 1024 * 1024
CHUNKS = 4
GROUPS = 2


def layer_normalize(inputs, scale_gain):
    sample_expectation = jnp.mean(inputs, axis=-1, keepdims=True)
    centered = inputs - sample_expectation
    variance = jnp.mean(centered * centered, axis=-1, keepdims=True)
    return centered * lax.rsqrt(variance + 1e-05) * scale_gain


def dot_f32(a, b, ca, cb):
    return lax.dot_general(a, b, (((ca,), (cb,)), ((), ())), preferred_element_type=jnp.float32)


def sequence_kernel(
    heads,
    pack,
    blocks,
    *refs,
):
    rank_ref, refs = refs[0], refs[1:]
    x_refs, refs = refs[:blocks], refs[blocks:]
    weight_refs, refs = refs[:11], refs[11:]
    out_refs, (right_ref, gathered, left_acc, right_acc) = refs[:blocks], refs[blocks:]
    (
        bias_ref,
        gain_ref,
        probe_ref,
        offset_ref,
        final_ref,
        ff_gain_ref,
        widen_ref,
        shrink_ref,
        opm_gain_ref,
        left_w_ref,
        right_w_ref,
    ) = weight_refs
    rank = rank_ref[0]
    step = pl.program_id(0)
    steps = right_ref.shape[2]
    _, rows, width = x_refs[0].shape
    length = blocks * rows
    depth = width // heads
    for d in range(blocks):
        gathered[lax.rem(rank + blocks - d, blocks)] = x_refs[d][0]
    x = gathered[...].astype(jnp.float32).reshape(length, width)
    normed = layer_normalize(x, gain_ref[...]).astype(jnp.bfloat16)
    mapped = dot_f32(probe_ref[...], normed, 1, 1)
    q = (mapped[:width] * (depth ** (-0.5) * LOG2E)).astype(jnp.bfloat16)
    k = mapped[width : 2 * width].astype(jnp.bfloat16)
    v = mapped[2 * width : 3 * width].astype(jnp.bfloat16)
    gate = jax.nn.sigmoid(mapped[3 * width :] + offset_ref[...])
    def due(s):
        early = steps - AHEAD
        slow = early * SLOW // 10
        return jnp.where(s <= early, s * SLOW // 10, slow + (s - early) * FAST // 10)

    def send_back_upto(first, end):
        def one(s, carry):
            send_back(s)
            return carry

        lax.fori_loop(first, end, one, 0)

    ones = jnp.ones((16, length), jnp.bfloat16)
    gated = []
    for h in range(heads):
        part = slice(h * depth, (h + 1) * depth)
        scores = dot_f32(k[part], q[part], 0, 0) + bias_ref[h]
        top = jnp.max(scores, axis=0, keepdims=True)
        p = jnp.exp2(scores - top).astype(jnp.bfloat16)
        mixed = dot_f32(jnp.concatenate([v[part], ones], axis=0), p, 1, 0)
        share = mixed[:depth] / mixed[depth : depth + 1]
        gated.append((share * gate[part]).astype(jnp.bfloat16))
    gated = jnp.concatenate(gated, axis=0)
    stream = x + dot_f32(gated, final_ref[...], 0, 0)
    normed = layer_normalize(stream, ff_gain_ref[...]).astype(jnp.bfloat16)
    hidden = jnp.maximum(dot_f32(normed, widen_ref[...], 1, 0), 0.0).astype(jnp.bfloat16)
    stream = stream + dot_f32(hidden, shrink_ref[...], 1, 0)
    updated = stream.astype(jnp.bfloat16)
    gathered[...] = stream.reshape(blocks, rows, width).astype(jnp.bfloat16)
    for d in range(blocks):
        out_refs[d][step] = gathered[lax.rem(rank + d, blocks)]
    normed = layer_normalize(updated.astype(jnp.float32), opm_gain_ref[...]).astype(jnp.bfloat16)
    slot = lax.rem(step, pack)
    left = dot_f32(normed, left_w_ref[slot], 1, 0).reshape(left_acc.shape)

    @pl.when(slot == 0)
    def _():
        left_acc[...] = left

    @pl.when(slot != 0)
    def _():
        left_acc[...] = left_acc[...] + left

    factor = right_w_ref.shape[0]
    right = dot_f32(right_w_ref[...], normed, 1, 1)
    for e in range(factor):
        right_acc[e, pl.ds(step, 1), :] = right[e : e + 1]

    @pl.when(step == steps - 1)
    def _():
        lanes = left_acc.shape[2]
        cols = right_ref.shape[3]
        for part in range(right_ref.shape[0]):
            right_ref[part] = right_acc[:, :, part * cols : (part + 1) * cols].astype(jnp.bfloat16)
        for d in range(blocks):
            if lanes < width:
                out_refs[d][steps] = jnp.zeros((rows, width), jnp.bfloat16)
            out_refs[d][steps, :, :lanes] = left_acc[lax.rem(rank + d, blocks)].astype(jnp.bfloat16)


def run_sequences(rank, xs, bias, weights, heads, pack, halves):
    blocks = len(xs)
    steps, rows, width = xs[0].shape
    length = blocks * rows
    factor = weights[-1].shape[0]
    cols = length // halves
    whole = lambda a: pl.BlockSpec(
        a.shape, lambda s, n=a.ndim: (0,) * n, pipeline_mode=pl.Buffered(1)
    )
    kept = lambda shape: pl.BlockSpec(shape, lambda s, n=len(shape): (0,) * n)
    lanes = pack * factor
    hidden = weights[5].shape[1]
    flops = 2 * length * width * (5 * width + 2 * hidden + 128) + 4 * length * length * width
    shapes = [(steps + 1, rows, width)] * blocks + [(halves, factor, steps, cols)]
    return pl.pallas_call(
        functools.partial(sequence_kernel, heads, pack, blocks),
        grid=(steps,),
        in_specs=[pl.BlockSpec(memory_space=pltpu.SMEM)]
        + [pl.BlockSpec((1, rows, width), lambda s: (s, 0, 0)) for _ in xs]
        + [whole(a) for a in (bias,) + weights],
        out_specs=[kept(a) for a in shapes],
        out_shape=[jax.ShapeDtypeStruct(a, jnp.bfloat16) for a in shapes],
        scratch_shapes=[
            pltpu.VMEM((blocks, rows, width), jnp.bfloat16),
            pltpu.VMEM((blocks, rows, lanes), jnp.float32),
            pltpu.VMEM((factor, steps, length), jnp.float32),
        ],
        compiler_params=pltpu.CompilerParams(
            dimension_semantics=("arbitrary",), vmem_limit_bytes=VMEM_LIMIT
        ),
        cost_estimate=pl.CostEstimate(
            flops=steps * flops * 3,
            bytes_accessed=bias.size * 4 + 4 * length * width * steps,
            transcendentals=steps * heads * length * length,
        ),
        name="sequences",
    )(rank, *xs, bias, *weights)


def deal_kernel(chunks, rank_ref, x_ref, *out_refs):
    blocks = x_ref.shape[0]
    part = x_ref.shape[1] // chunks
    for c in range(chunks):
        for d in range(blocks):
            source = lax.rem(rank_ref[0] + d, blocks)
            out_refs[c * blocks + d][...] = x_ref[source, c * part : (c + 1) * part]


def collect_kernel(chunks, rank_ref, *refs):
    in_refs, (out_ref, left_ref) = refs[:-2], refs[-2:]
    blocks = out_ref.shape[0]
    part = out_ref.shape[1] // chunks
    lanes = left_ref.shape[3]
    for c in range(chunks):
        for d in range(blocks):
            target = lax.rem(rank_ref[0] + blocks - d, blocks)
            y_ref = in_refs[c * blocks + d]
            out_ref[target, c * part : (c + 1) * part] = y_ref[:part]
            left_ref[target, c] = y_ref[part, :, :lanes]


def vmem_call(kernel, shapes, rank, arrays, name):
    return pl.pallas_call(
        kernel,
        in_specs=[pl.BlockSpec(memory_space=pltpu.SMEM)]
        + [pl.BlockSpec(memory_space=pltpu.VMEM)] * len(arrays),
        out_specs=[pl.BlockSpec(memory_space=pltpu.VMEM)] * len(shapes),
        out_shape=[jax.ShapeDtypeStruct(a, jnp.bfloat16) for a in shapes],
        compiler_params=pltpu.CompilerParams(vmem_limit_bytes=VMEM_LIMIT // 2),
        cost_estimate=pl.CostEstimate(
            flops=0, bytes_accessed=4 * sum(a.size for a in arrays), transcendentals=0
        ),
        name=name,
    )(rank, *arrays)


def shift_all(arrays):
    size = len(arrays)
    return [arrays[0]] + [
        lax.ppermute(arrays[d], "res", [(r, (r + d) % size) for r in range(size)])
        for d in range(1, size)
    ]


def product_kernel(rows, seq_total, left_ref, *refs):
    right_refs, (table_ref, pair_ref, out_ref, stack) = refs[:-4], refs[-4:]
    groups, factor, part, cols = right_refs[0].shape
    scale = 1.0 / seq_total
    left = left_ref[...]
    for e in range(factor):
        right = jnp.concatenate(
            [ref[:, e].reshape(groups * part, cols) for ref in right_refs], axis=0
        )
        outer = (dot_f32(left, right, 1, 0) * scale).astype(jnp.bfloat16)
        stack[:, e * factor : (e + 1) * factor, :] = outer.reshape(rows, factor, cols)
    for i in range(rows):
        update = dot_f32(table_ref[...], stack[i], 1, 0)
        out_ref[i] = (pair_ref[i].astype(jnp.float32) + update.T).astype(jnp.bfloat16)


def run_product(left, rights, table, pair):
    total_rows, seq_total = left.shape
    _, factor, _, cols = rights[0].shape
    pair_rows = pair.shape[0]
    rows = math.gcd(pair_rows, 8)
    width = pair.shape[2]
    return pl.pallas_call(
        functools.partial(product_kernel, rows, seq_total),
        grid=(pair_rows // rows,),
        in_specs=[
            pl.BlockSpec((rows * factor, seq_total), lambda b: (b, 0)),
            *[
                pl.BlockSpec(a.shape, lambda b: (0, 0, 0, 0), pipeline_mode=pl.Buffered(1))
                for a in rights
            ],
            pl.BlockSpec(table.shape, lambda b: (0, 0), pipeline_mode=pl.Buffered(1)),
            pl.BlockSpec((rows, cols, width), lambda b: (b, 0, 0)),
        ],
        out_specs=pl.BlockSpec((rows, cols, width), lambda b: (b, 0, 0)),
        out_shape=jax.ShapeDtypeStruct(pair.shape, jnp.bfloat16),
        scratch_shapes=[pltpu.VMEM((rows, factor * factor, cols), jnp.bfloat16)],
        compiler_params=pltpu.CompilerParams(
            dimension_semantics=("arbitrary",), vmem_limit_bytes=VMEM_LIMIT
        ),
        cost_estimate=pl.CostEstimate(
            flops=4 * total_rows * cols * factor * (seq_total + width),
            bytes_accessed=2 * (left.size * (1 + cols * factor // total_rows) + left.size + 2 * pair.size),
            transcendentals=0,
        ),
        name="product",
    )(left, *rights, table, pair)


def permuted_on_device(
    aligned_activity,
    pair_state,
    focus_scaling_vector,
    combined_probe_matrix,
    sigmoid_offset_vector,
    focus_final_matrix,
    pair_norm_gain,
    pair_bias_matrix,
    feedforward_scaling_vector,
    feedforward_widen_matrix,
    feedforward_shrink_matrix,
    tensor_scaling_vector,
    twin_operand_matrix,
    tensor_final_matrix,
):
    width = aligned_activity.shape[2]
    heads = pair_bias_matrix.shape[1]
    factor = twin_operand_matrix.shape[1] // 2
    res_axis = lax.axis_size("res")
    seq_axis = lax.axis_size("seq")
    rows = aligned_activity.shape[1]
    seq_count = aligned_activity.shape[0] // res_axis
    length = rows * res_axis
    col_block = pair_state.shape[1]
    chunks = math.gcd(CHUNKS, seq_count)
    per_chunk = seq_count // chunks
    pack = per_chunk

    groups = math.gcd(GROUPS, chunks) if seq_count % (8 * GROUPS) == 0 else 1
    rank = lax.axis_index("res").astype(jnp.int32).reshape(1)
    pieces = aligned_activity.reshape(res_axis, seq_count, rows, width)
    dealt = vmem_call(
        functools.partial(deal_kernel, chunks),
        [(per_chunk, rows, width)] * (chunks * res_axis),
        rank,
        [pieces],
        "deal",
    )
    arrived = [shift_all(dealt[c * res_axis : (c + 1) * res_axis]) for c in range(chunks)]

    pair_norm = layer_normalize(pair_state.astype(jnp.float32), pair_norm_gain)
    bias_tile = jnp.einsum(
        "ijc,ch->hij", pair_norm, pair_bias_matrix, precision=lax.Precision.HIGHEST
    ).astype(jnp.bfloat16)
    bias_rows = lax.all_gather(bias_tile, "res", axis=1, tiled=True)
    bias_all = lax.all_gather(bias_rows, "seq", axis=0)
    bias = bias_all.transpose(1, 0, 3, 2).reshape(heads, length, length)
    bias = bias.astype(jnp.float32) * LOG2E

    left_w = twin_operand_matrix[:, :factor]
    left_w = jnp.stack(
        [jnp.pad(left_w, ((0, 0), (t * factor, (pack - 1 - t) * factor))) for t in range(pack)]
    )
    weights = (
        focus_scaling_vector.reshape(1, -1),
        combined_probe_matrix.T,
        sigmoid_offset_vector.reshape(-1, 1),
        focus_final_matrix,
        feedforward_scaling_vector.reshape(1, -1),
        feedforward_widen_matrix,
        feedforward_shrink_matrix,
        tensor_scaling_vector.reshape(1, -1),
        left_w,
        twin_operand_matrix[:, factor:].T,
    )
    returned, rights, pending = [], [], []
    for c in range(chunks):
        *updated, right = run_sequences(rank, arrived[c], bias, weights, heads, pack, seq_axis)
        returned += shift_all(updated)
        pending.append(right)
        if len(pending) == chunks // groups:
            right = jnp.concatenate(pending, axis=2)
            right = lax.all_to_all(right, "seq", split_axis=0, concat_axis=0, tiled=True)
            rights.append(lax.all_gather(right, "res", axis=0, tiled=True))
            pending = []
    if (seq_count // groups) % 8 != 0:
        rights = [r.transpose(1, 0, 2, 3).reshape(1, factor, -1, col_block) for r in rights]
    alignment_output, left = vmem_call(
        functools.partial(collect_kernel, chunks),
        [pieces.shape, (res_axis, chunks, rows, pack * factor)],
        rank,
        returned,
        "collect",
    )
    alignment_output = alignment_output.reshape(aligned_activity.shape)
    left = lax.all_gather(left, "seq", axis=0)
    left = left.reshape(seq_axis, res_axis, groups, chunks // groups, rows, pack, factor)
    left = left.transpose(4, 6, 2, 1, 0, 3, 5).reshape(rows * factor, -1)

    table = tensor_final_matrix.reshape(factor, factor, -1).transpose(2, 1, 0)
    table = table.reshape(table.shape[0], -1)
    pair_output = run_product(left, rights, table, pair_state)
    return (alignment_output, pair_output)


MESH = pl.DeviceIdType.MESH
GROUP = 8
AHEAD = 7
FIRST = 3
FILL = 0
SLOW = 2
FAST = 12
LANES = 128


def dot_t(a, b):
    return dot_f32(a, b, 1, 1)


def wait_for(ref, sem):
    pltpu.make_async_copy(ref, ref, sem).wait()


def send(src, dst, sent, arrived, **peer):
    pltpu.make_async_remote_copy(
        src_ref=src,
        dst_ref=dst,
        send_sem=sent,
        recv_sem=arrived,
        device_id=peer,
        device_id_type=MESH,
    ).start()


class Relay:
    def __init__(self, rank, deep, wide, tile, tiles, arrived, sent_z, sent_x, forward=None):
        self.rank, self.deep, self.wide = rank, deep, wide
        self.z, self.x = rank // wide, rank % wide
        self.tile, self.tiles, self.arrived = tile, tiles, arrived
        self.sent_z, self.sent_x, self.forward = sent_z, sent_x, forward

    def pass_on(self, owner):
        for d in range(1, self.wide):
            peer = self.z * self.wide + (self.x + d) % self.wide
            send(self.tile(owner), self.tile(owner), self.sent_x, self.arrived.at[owner], res=peer)
        if self.forward is not None:
            self.forward(owner)

    def ends(self, hop, way):
        z = self.z - hop if way == 0 else self.z + hop
        there = z >= 0 if way == 0 else z < self.deep
        onward = self.z + 1 < self.deep if way == 0 else self.z >= 1
        peer = self.rank + self.wide if way == 0 else self.rank - self.wide
        return z * self.wide + self.x, there, onward, peer

    def start(self):
        for way in range(2):
            owner, _, onward, peer = self.ends(0, way)

            @pl.when(onward)
            def _():
                send(
                    self.tile(self.rank),
                    self.tile(self.rank),
                    self.sent_z.at[0, way],
                    self.arrived.at[self.rank],
                    res=peer,
                )

        self.pass_on(self.rank)

    def hop(self, hop):
        for way in range(2):
            owner, there, onward, peer = self.ends(hop, way)

            @pl.when(there)
            def _():
                wait_for(self.tile(owner), self.arrived.at[owner])

                @pl.when(onward)
                def _():
                    send(
                        self.tile(owner),
                        self.tile(owner),
                        self.sent_z.at[hop, way],
                        self.arrived.at[owner],
                        res=peer,
                    )

                self.pass_on(owner)

    def across(self):
        for d in range(1, self.wide):
            for z in range(self.deep):
                owner = z * self.wide + (self.x + d) % self.wide
                wait_for(self.tile(owner), self.arrived.at[owner])
                if self.forward is not None:
                    self.forward(owner)

    def finish(self):
        for hop in range(self.deep):
            for way in range(2):
                owner, there, onward, _ = self.ends(hop, way)

                @pl.when(jnp.logical_and(there, onward))
                def _():
                    wait_for(self.tile(owner), self.sent_z.at[hop, way])

        for d in range(1, self.wide):
            wait_for(self.tiles(self.deep), self.sent_x)


def fused_kernel(heads, ranks, wide, x_ref, pair_ref, *refs):
    given, refs = refs[:12], refs[12:]
    (out_ref, pair_out_ref), refs = refs[:2], refs[2:]
    held, refs = refs[:12], refs[12:]
    (
        gain_ref,
        probe_rows,
        offset_row,
        final_ref,
        ff_gain_ref,
        widen_ref,
        shrink_ref,
        opm_gain_ref,
        twin_ref,
        pair_gain_ref,
        pair_w_ref,
        table_rows,
    ) = held
    (
        xbuf,
        pairv,
        early,
        tile_s,
        tiles,
        bias,
        acc,
        left_acc,
        stage,
        right_v,
        left_out,
        left_in,
        left_s,
        left_t,
        normal,
        left_v,
        stack,
        probe_ref,
        offset_ref,
        table_s,
        table_ref,
    ), sems = refs[:21], refs[21:]
    (
        pair_sem,
        held_sem,
        x_in,
        x_out,
        ret_in,
        ret_out,
        tile_in,
        tile_z,
        tile_x,
        twin_out,
        twin_in,
        right_in,
        right_z,
        right_x,
        half_out,
        half_in,
        half_own,
        left_sem,
    ) = sems
    rank = lax.axis_index("res")
    core = lax.axis_index("seq")
    blocks, steps, rows, width = xbuf.shape
    length = blocks * rows
    depth = width // heads
    factor = twin_ref.shape[0] // 2
    cols = length // 2
    spans = steps // GROUP
    deep = ranks // wide

    barrier = pltpu.get_barrier_semaphore()
    for d in range(1, blocks):
        pl.semaphore_signal(
            barrier, inc=1, device_id={"res": (rank + d) % blocks}, device_id_type=MESH
        )
    pl.semaphore_signal(barrier, inc=1, device_id={"seq": 1 - core}, device_id_type=MESH)
    pl.semaphore_wait(barrier, blocks)

    def send_x(s):
        for d in range(1, blocks):
            to = (rank + d) % blocks
            send(x_ref.at[to * steps + s], xbuf.at[rank, s], x_out.at[0], x_in.at[s], res=to)
        pltpu.make_async_copy(x_ref.at[rank * steps + s], xbuf.at[rank, s], x_in.at[s]).start()

    def send_back(s):
        def all_to(target, arrived):
            for d in range(1, blocks):
                to = (rank + d) % blocks
                send(xbuf.at[to, s], target, ret_out.at[0], arrived, res=to)
            pltpu.make_async_copy(xbuf.at[rank, s], target, arrived).start()

        @pl.when(s < GROUP)
        def _():
            all_to(early.at[rank, s], ret_in.at[0])

        @pl.when(s >= GROUP)
        def _():
            all_to(out_ref.at[rank * steps + s], ret_in.at[1])

    pair_copy = pltpu.make_async_copy(pair_ref, pairv, pair_sem.at[0])
    pair_copy.start()
    for s in range(FIRST):
        send_x(s)
    copies = [
        pltpu.make_async_copy(given[i], held[i], held_sem.at[i]) for i in range(len(given))
    ]
    for copy in copies:
        copy.start()
    for copy in copies:
        copy.wait()
    pair_copy.wait()

    def tile_rows(i, carry):
        values = pairv[i].astype(jnp.float32)
        normed = layer_normalize(values, pair_gain_ref[...])
        tile = lax.dot_general(
            pair_w_ref[...],
            normed,
            (((1,), (1,)), ((), ())),
            precision=lax.Precision.HIGHEST,
            preferred_element_type=jnp.float32,
        )
        for h in range(heads):
            tile_s[h, pl.ds(i, 1), :] = tile[h : h + 1]
        return carry

    lax.fori_loop(0, rows, tile_rows, 0, unroll=4)
    pack = LANES // rows
    for p in range(heads // pack):
        both = tile_s[p * pack : (p + 1) * pack].reshape(LANES, cols)
        tiles[core, rank, p] = both.T.astype(jnp.bfloat16)

    def to_twin(owner):
        send(
            tiles.at[core, owner], tiles.at[core, owner], twin_out.at[0], twin_in.at[0], seq=1 - core
        )

    spread = Relay(
        rank,
        deep,
        wide,
        lambda o: tiles.at[core, o],
        lambda c: tiles.at[core, pl.ds(0, c)],
        tile_in,
        tile_z,
        tile_x.at[0],
        to_twin,
    )

    def prepare():
        for c in range(0, probe_rows.shape[1], width):
            columns = probe_rows[:, c : c + width].astype(jnp.float32)
            probe_ref[c : c + width] = columns.T.astype(jnp.bfloat16)
        offset_ref[...] = jnp.broadcast_to(offset_row[...], (LANES, width)).T
        table_s[...] = table_rows[...].astype(jnp.float32)
        few = LANES // factor
        for e in range(0, factor, few):
            lines = [table_s[pl.ds(e + i, factor, stride=factor), :] for i in range(few)]
            lines = jnp.concatenate(lines, axis=0)
            table_ref[:, e * factor : (e + few) * factor] = lines.T.astype(jnp.bfloat16)

    spread.start()
    send_x(FIRST)
    prepare()
    for hop in range(1, deep):
        spread.hop(hop)
        if FIRST + hop < AHEAD:
            send_x(FIRST + hop)
    for s in range(min(FIRST + deep, AHEAD), AHEAD):
        send_x(s)
    spread.across()
    wait_for(tiles.at[1 - core], twin_in.at[0])

    low = lax.broadcasted_iota(jnp.int32, (cols, LANES), 1) < rows

    def fill(step, carry):
        half, p = step // (heads // pack), step % (heads // pack)
        for k in range(blocks // pack):
            even = tiles[half, pack * k, p].astype(jnp.float32) * LOG2E
            odd = tiles[half, pack * k + 1, p].astype(jnp.float32) * LOG2E
            here = (pl.ds(pl.multiple_of(half * cols, cols), cols), slice(k * LANES, (k + 1) * LANES))
            bias[(pack * p,) + here] = jnp.where(low, even, pltpu.roll(odd, rows, 1))
            bias[(pack * p + 1,) + here] = jnp.where(low, pltpu.roll(even, rows, 1), odd)
        return carry

    lax.fori_loop(0, 2 * heads // pack, fill, 0)

    def relay_of(u):
        return Relay(
            rank,
            deep,
            wide,
            lambda o: right_v.at[:, u, o],
            lambda c: right_v.at[:, u, pl.ds(0, c)],
            right_in.at[u],
            right_z.at[u],
            right_x.at[u],
        )

    def swap_halves(u):
        send(stage.at[u, 1], right_v.at[core, u, rank], half_out.at[u], half_in.at[u], seq=1 - core)
        pltpu.make_async_copy(stage.at[u, 0], right_v.at[core, u, rank], half_own.at[u]).start()

    def start_right(u):
        wait_for(right_v.at[core, u, rank], half_own.at[u])
        wait_for(right_v.at[1 - core, u, rank], half_in.at[u])
        relay_of(u).start()

    def due(s):
        early = steps - AHEAD
        slow = early * SLOW // 10
        return jnp.where(s <= early, s * SLOW // 10, slow + (s - early) * FAST // 10)

    def send_back_upto(first, end):
        def one(s, carry):
            send_back(s)
            return carry

        lax.fori_loop(first, end, one, 0)

    ones = jnp.ones((16, length), jnp.bfloat16)

    def sequence(s, carry):
        wait_for(xbuf.at[:, s], x_in.at[s])

        @pl.when(s + AHEAD < steps)
        def _():
            send_x(s + AHEAD)

        u, place = s // GROUP - 1, s % GROUP

        @pl.when(jnp.logical_and(u >= 0, place == 0))
        def _():
            swap_halves(u)

        send_back_upto(due(s), due(s + 1))

        @pl.when(jnp.logical_and(u >= 0, place == 1))
        def _():
            start_right(u)

        @pl.when(jnp.logical_and(u >= 0, jnp.logical_and(place > 1, place % 2 == 1)))
        def _():
            relay_of(u).hop(place // 2)

        x = xbuf[:, s].astype(jnp.float32).reshape(length, width)
        normed = layer_normalize(x, gain_ref[...]).astype(jnp.bfloat16)
        mapped = dot_t(probe_ref[...], normed)
        q = (mapped[:width] * (depth ** (-0.5) * LOG2E)).astype(jnp.bfloat16)
        k = mapped[width : 2 * width].astype(jnp.bfloat16)
        v = mapped[2 * width : 3 * width].astype(jnp.bfloat16)
        gate = jax.nn.sigmoid(mapped[3 * width :] + offset_ref[:, :1])
        gated = []
        for h in range(heads):
            part = slice(h * depth, (h + 1) * depth)
            scores = dot_f32(k[part], q[part], 0, 0) + bias[h]
            top = jnp.max(scores, axis=0, keepdims=True)
            p = jnp.exp2(scores - top).astype(jnp.bfloat16)
            mixed = dot_f32(jnp.concatenate([v[part], ones], axis=0), p, 1, 0)
            share = mixed[:depth] / mixed[depth : depth + 1]
            gated.append((share * gate[part]).astype(jnp.bfloat16))
        gated = jnp.concatenate(gated, axis=0)
        stream = x + dot_f32(gated, final_ref[...], 0, 0)
        normed = layer_normalize(stream, ff_gain_ref[...]).astype(jnp.bfloat16)
        hidden = jnp.maximum(dot_f32(normed, widen_ref[...], 1, 0), 0.0).astype(jnp.bfloat16)
        stream = stream + dot_f32(hidden, shrink_ref[...], 1, 0)
        updated = stream.astype(jnp.bfloat16)
        xbuf[:, s] = stream.reshape(blocks, rows, width).astype(jnp.bfloat16)
        normed = layer_normalize(updated.astype(jnp.float32), opm_gain_ref[...]).astype(jnp.bfloat16)
        factors = dot_t(twin_ref[...], normed)
        for e in range(factor):
            left_acc[e, pl.ds(place, 1), :] = factors[e : e + 1]
            acc[e, pl.ds(place, 1), :] = factors[factor + e : factor + e + 1]

        @pl.when(place == GROUP - 1)
        def _():
            own = pl.ds(pl.multiple_of(core * cols, cols), cols)
            other = pl.ds(pl.multiple_of((1 - core) * cols, cols), cols)
            stage[u + 1, 0] = acc[:, :, own].astype(jnp.bfloat16)
            stage[u + 1, 1] = acc[:, :, other].astype(jnp.bfloat16)

        return carry

    lax.fori_loop(0, steps, sequence, 0)

    last = spans - 1
    sent = due(steps)
    swap_halves(last)
    pairs = factor // 2
    near = lax.broadcasted_iota(jnp.int32, (pairs, GROUP, LANES), 2) < rows
    for m in range(blocks // 2):
        lanes = slice(m * LANES, (m + 1) * LANES)
        one, two = left_acc[:pairs, :, lanes], left_acc[pairs:, :, lanes]
        left_out[2 * m] = jnp.where(near, one, pltpu.roll(two, rows, 2)).astype(jnp.bfloat16)
        left_out[2 * m + 1] = jnp.where(near, pltpu.roll(one, rows, 2), two).astype(jnp.bfloat16)
    start_right(last)
    for d in range(1, blocks):
        to = (rank + d) % blocks
        send(left_out.at[to], left_in.at[rank], left_sem.at[0], left_sem.at[1], res=to)
    pltpu.make_async_copy(left_out.at[rank], left_in.at[rank], left_sem.at[1]).start()

    def normalize(b, carry):
        values = early[b].astype(jnp.float32).reshape(-1, width)
        values = layer_normalize(values, opm_gain_ref[...]).astype(jnp.bfloat16)
        place = pl.ds(pl.multiple_of(b * GROUP * rows, GROUP * rows), GROUP * rows)
        for c in range(width // LANES):
            lanes = values[:, c * LANES : (c + 1) * LANES]
            normal[c, place, :] = lanes.astype(jnp.float32)
        return carry

    def left_rows(i, carry):
        values = [
            normal[c, pl.ds(i, blocks * GROUP, stride=rows), :].astype(jnp.bfloat16)
            for c in range(width // LANES)
        ]
        values = dot_t(twin_ref[:factor], jnp.concatenate(values, axis=1))
        left_s[pl.ds(pl.multiple_of(i * factor, factor), factor), : LANES // 2] = values
        return carry

    def early_left():
        wait_for(early, ret_in.at[0])
        for b in range(blocks):
            target = out_ref.at[pl.ds(b * steps, GROUP)]
            pltpu.make_async_copy(early.at[b], target, ret_in.at[2]).start()
        lax.fori_loop(0, blocks, normalize, 0)
        lax.fori_loop(0, rows, left_rows, 0, unroll=8)

    for hop in range(1, deep):
        relay_of(last).hop(hop)
        send_back_upto(sent + (hop - 1) * FILL, sent + hop * FILL)
    send_back_upto(sent + (deep - 1) * FILL, steps)
    early_left()

    wait_for(left_in, left_sem.at[1])
    for c in range(pairs):
        values = left_in[:, c].astype(jnp.float32).reshape(blocks * GROUP, LANES).T
        values = jnp.concatenate([values, values], axis=1)
        for half in range(2):
            part = values[half * rows : (half + 1) * rows]
            left_t[pl.ds(half * pairs + c, rows, stride=factor), :] = part
    first = lax.broadcasted_iota(jnp.int32, left_s.shape, 1) < LANES // 2
    left_v[core] = jnp.where(first, left_s[...], left_t[...]).astype(jnp.bfloat16)
    send(left_v.at[core], left_v.at[core], left_sem.at[2], left_sem.at[3], seq=1 - core)
    for u in range(spans):
        relay_of(u).across()
    wait_for(left_v.at[1 - core], left_sem.at[3])

    some = stack.shape[0]
    scale = 1.0 / (2 * blocks * steps)

    def pair_block(b, carry):
        place = pl.ds(pl.multiple_of(b * some * factor, some * factor), some * factor)
        left = jnp.concatenate([left_v[0, place, :], left_v[1, place, :]], axis=1)
        for e in range(factor):
            right = right_v[:, :, :, e].reshape(2 * blocks * steps, cols)
            outer = (dot_f32(left, right, 1, 0) * scale).astype(jnp.bfloat16)
            stack[:, e * factor : (e + 1) * factor, :] = outer.reshape(some, factor, cols)
        for i in range(some):
            update = dot_f32(table_ref[...], stack[i], 1, 0)
            at = b * some + i
            pairv[at] = (pairv[at].astype(jnp.float32) + update.T).astype(jnp.bfloat16)
        these = pl.ds(b * some, some)
        pltpu.make_async_copy(pairv.at[these], pair_out_ref.at[these], pair_sem.at[1]).start()
        return carry

    lax.fori_loop(0, rows // some, pair_block, 0)

    wait_for(x_ref.at[pl.ds(0, (blocks - 1) * steps)], x_out.at[0])
    wait_for(out_ref.at[pl.ds(0, (blocks - 1) * steps)], ret_out.at[0])
    spread.finish()
    wait_for(tiles.at[core], twin_out.at[0])
    for u in range(spans):
        relay_of(u).finish()
        wait_for(stage.at[u, 1], half_out.at[u])
    wait_for(left_out.at[pl.ds(0, blocks - 1)], left_sem.at[0])
    wait_for(left_v.at[core], left_sem.at[2])
    wait_for(out_ref.at[pl.ds(0, blocks * (steps - GROUP))], ret_in.at[1])
    wait_for(early, ret_in.at[2])
    wait_for(pairv, pair_sem.at[1])


def run_fused(x, pair, weights, heads, ranks, wide):
    sequences, rows, width = x.shape
    steps = sequences // ranks
    length = rows * ranks
    cols = pair.shape[1]
    factor = weights[8].shape[0] // 2
    spans = steps // GROUP
    deep = ranks // wide
    pack = LANES // rows
    table = weights[11].shape
    any_spec = pl.BlockSpec(memory_space=pl.ANY)
    dma = lambda *shape: pltpu.SemaphoreType.DMA(shape)
    half = lambda *shape: pltpu.VMEM(shape, jnp.bfloat16)
    full = lambda *shape: pltpu.VMEM(shape, jnp.float32)
    return pl.pallas_call(
        functools.partial(fused_kernel, heads, ranks, wide),
        in_specs=[any_spec] * (2 + len(weights)),
        out_specs=[any_spec] * 2,
        out_shape=[jax.ShapeDtypeStruct(a, jnp.bfloat16) for a in (x.shape, pair.shape)],
        scratch_shapes=[pltpu.VMEM(a.shape, a.dtype) for a in weights]
        + [
            half(ranks, steps, rows, width),
            half(*pair.shape),
            half(ranks, GROUP, rows, width),
            full(heads, rows, cols),
            half(2, ranks, heads // pack, cols, LANES),
            full(heads, length, length),
            full(factor, GROUP, length),
            full(factor, GROUP, length),
            half(spans, 2, factor, GROUP, cols),
            half(2, spans, ranks, factor, GROUP, cols),
            half(ranks, factor // 2, GROUP, LANES),
            half(ranks, factor // 2, GROUP, LANES),
            full(rows * factor, LANES),
            full(rows * factor, LANES),
            full(width // LANES, ranks * GROUP * rows, LANES),
            half(2, rows * factor, LANES),
            half(math.gcd(rows, 8), factor * factor, cols),
            half(4 * width, width),
            full(width, LANES),
            full(*table),
            half(table[1], table[0]),
            dma(2),
            dma(len(weights)),
            dma(steps),
            dma(1),
            dma(3),
            dma(1),
            dma(ranks),
            dma(deep, 2),
            dma(1),
            dma(1),
            dma(1),
            dma(spans, ranks),
            dma(spans, deep, 2),
            dma(spans),
            dma(spans),
            dma(spans),
            dma(spans),
            dma(4),
        ],
        compiler_params=pltpu.CompilerParams(
            vmem_limit_bytes=FUSED_VMEM, collective_id=0, has_side_effects=True
        ),
        name="fused",
    )(x, pair, *weights)


def fits(rows, steps, ranks, heads, seq_axis):
    return (
        seq_axis == 2
        and rows * 2 == LANES
        and heads % 2 == 0
        and ranks % 2 == 0
        and steps == 2 * GROUP
        and ranks == GROUP
        and steps >= AHEAD
    )


def fused_on_device(
    aligned_activity,
    pair_state,
    focus_scaling_vector,
    combined_probe_matrix,
    sigmoid_offset_vector,
    focus_final_matrix,
    pair_norm_gain,
    pair_bias_matrix,
    feedforward_scaling_vector,
    feedforward_widen_matrix,
    feedforward_shrink_matrix,
    tensor_scaling_vector,
    twin_operand_matrix,
    tensor_final_matrix,
):
    heads = pair_bias_matrix.shape[1]
    weights = (
        focus_scaling_vector.reshape(1, -1),
        combined_probe_matrix,
        sigmoid_offset_vector.reshape(1, -1),
        focus_final_matrix,
        feedforward_scaling_vector.reshape(1, -1),
        feedforward_widen_matrix,
        feedforward_shrink_matrix,
        tensor_scaling_vector.reshape(1, -1),
        twin_operand_matrix.T,
        pair_norm_gain.reshape(1, -1),
        pair_bias_matrix.T,
        tensor_final_matrix,
    )
    return tuple(
        run_fused(aligned_activity, pair_state, weights, heads, lax.axis_size("res"), 2)
    )


def on_device(aligned_activity, pair_state, *parameters):
    ranks = lax.axis_size("res")
    rows = aligned_activity.shape[1]
    steps = aligned_activity.shape[0] // ranks
    heads = parameters[5].shape[1]
    if fits(rows, steps, ranks, heads, lax.axis_size("seq")):
        return fused_on_device(aligned_activity, pair_state, *parameters)
    return permuted_on_device(aligned_activity, pair_state, *parameters)


def solution(mesh):
    return jax.shard_map(
        on_device,
        mesh=mesh,
        in_specs=(
            P(("grp", "seq"), "res", None),
            P(("grp", "res"), "seq", None),
            P(),
            P(),
            P(),
            P(),
            P(),
            P(),
            P(),
            P(),
            P(),
            P(),
            P(),
            P(),
        ),
        out_specs=(P(("grp", "seq"), "res", None), P(("grp", "res"), "seq", None)),
        check_vma=False,
    )
```

```python
import functools
import math

import jax
import jax.numpy as jnp
from jax import lax
from jax.experimental import pallas as pl
from jax.experimental.pallas import tpu as pltpu
from jax.sharding import PartitionSpec as P

LOG2E = math.log2(math.e)
VMEM_LIMIT = 60 * 1024 * 1024
FUSED_VMEM = 54 * 1024 * 1024
CHUNKS = 4
GROUPS = 2


def layer_normalize(inputs, scale_gain):
    sample_expectation = jnp.mean(inputs, axis=-1, keepdims=True)
    centered = inputs - sample_expectation
    variance = jnp.mean(centered * centered, axis=-1, keepdims=True)
    return centered * lax.rsqrt(variance + 1e-05) * scale_gain


def dot_f32(a, b, ca, cb):
    return lax.dot_general(a, b, (((ca,), (cb,)), ((), ())), preferred_element_type=jnp.float32)


def sequence_kernel(
    heads,
    pack,
    blocks,
    *refs,
):
    rank_ref, refs = refs[0], refs[1:]
    x_refs, refs = refs[:blocks], refs[blocks:]
    weight_refs, refs = refs[:11], refs[11:]
    out_refs, (right_ref, gathered, left_acc, right_acc) = refs[:blocks], refs[blocks:]
    (
        bias_ref,
        gain_ref,
        probe_ref,
        offset_ref,
        final_ref,
        ff_gain_ref,
        widen_ref,
        shrink_ref,
        opm_gain_ref,
        left_w_ref,
        right_w_ref,
    ) = weight_refs
    rank = rank_ref[0]
    step = pl.program_id(0)
    steps = right_ref.shape[2]
    _, rows, width = x_refs[0].shape
    length = blocks * rows
    depth = width // heads
    for d in range(blocks):
        gathered[lax.rem(rank + blocks - d, blocks)] = x_refs[d][0]
    x = gathered[...].astype(jnp.float32).reshape(length, width)
    normed = layer_normalize(x, gain_ref[...]).astype(jnp.bfloat16)
    mapped = dot_f32(probe_ref[...], normed, 1, 1)
    q = (mapped[:width] * (depth ** (-0.5) * LOG2E)).astype(jnp.bfloat16)
    k = mapped[width : 2 * width].astype(jnp.bfloat16)
    v = mapped[2 * width : 3 * width].astype(jnp.bfloat16)
    gate = jax.nn.sigmoid(mapped[3 * width :] + offset_ref[...])
    def due(s):
        early = steps - AHEAD
        slow = early * SLOW // 10
        return jnp.where(s <= early, s * SLOW // 10, slow + (s - early) * FAST // 10)

    def send_back_upto(first, end):
        def one(s, carry):
            send_back(s)
            return carry

        lax.fori_loop(first, end, one, 0)

    ones = jnp.ones((16, length), jnp.bfloat16)
    gated = []
    for h in range(heads):
        part = slice(h * depth, (h + 1) * depth)
        scores = dot_f32(k[part], q[part], 0, 0) + bias_ref[h]
        top = jnp.max(scores, axis=0, keepdims=True)
        p = jnp.exp2(scores - top).astype(jnp.bfloat16)
        mixed = dot_f32(jnp.concatenate([v[part], ones], axis=0), p, 1, 0)
        share = mixed[:depth] / mixed[depth : depth + 1]
        gated.append((share * gate[part]).astype(jnp.bfloat16))
    gated = jnp.concatenate(gated, axis=0)
    stream = x + dot_f32(gated, final_ref[...], 0, 0)
    normed = layer_normalize(stream, ff_gain_ref[...]).astype(jnp.bfloat16)
    hidden = jnp.maximum(dot_f32(normed, widen_ref[...], 1, 0), 0.0).astype(jnp.bfloat16)
    stream = stream + dot_f32(hidden, shrink_ref[...], 1, 0)
    updated = stream.astype(jnp.bfloat16)
    gathered[...] = stream.reshape(blocks, rows, width).astype(jnp.bfloat16)
    for d in range(blocks):
        out_refs[d][step] = gathered[lax.rem(rank + d, blocks)]
    normed = layer_normalize(updated.astype(jnp.float32), opm_gain_ref[...]).astype(jnp.bfloat16)
    slot = lax.rem(step, pack)
    left = dot_f32(normed, left_w_ref[slot], 1, 0).reshape(left_acc.shape)

    @pl.when(slot == 0)
    def _():
        left_acc[...] = left

    @pl.when(slot != 0)
    def _():
        left_acc[...] = left_acc[...] + left

    factor = right_w_ref.shape[0]
    right = dot_f32(right_w_ref[...], normed, 1, 1)
    for e in range(factor):
        right_acc[e, pl.ds(step, 1), :] = right[e : e + 1]

    @pl.when(step == steps - 1)
    def _():
        lanes = left_acc.shape[2]
        cols = right_ref.shape[3]
        for part in range(right_ref.shape[0]):
            right_ref[part] = right_acc[:, :, part * cols : (part + 1) * cols].astype(jnp.bfloat16)
        for d in range(blocks):
            if lanes < width:
                out_refs[d][steps] = jnp.zeros((rows, width), jnp.bfloat16)
            out_refs[d][steps, :, :lanes] = left_acc[lax.rem(rank + d, blocks)].astype(jnp.bfloat16)


def run_sequences(rank, xs, bias, weights, heads, pack, halves):
    blocks = len(xs)
    steps, rows, width = xs[0].shape
    length = blocks * rows
    factor = weights[-1].shape[0]
    cols = length // halves
    whole = lambda a: pl.BlockSpec(
        a.shape, lambda s, n=a.ndim: (0,) * n, pipeline_mode=pl.Buffered(1)
    )
    kept = lambda shape: pl.BlockSpec(shape, lambda s, n=len(shape): (0,) * n)
    lanes = pack * factor
    hidden = weights[5].shape[1]
    flops = 2 * length * width * (5 * width + 2 * hidden + 128) + 4 * length * length * width
    shapes = [(steps + 1, rows, width)] * blocks + [(halves, factor, steps, cols)]
    return pl.pallas_call(
        functools.partial(sequence_kernel, heads, pack, blocks),
        grid=(steps,),
        in_specs=[pl.BlockSpec(memory_space=pltpu.SMEM)]
        + [pl.BlockSpec((1, rows, width), lambda s: (s, 0, 0)) for _ in xs]
        + [whole(a) for a in (bias,) + weights],
        out_specs=[kept(a) for a in shapes],
        out_shape=[jax.ShapeDtypeStruct(a, jnp.bfloat16) for a in shapes],
        scratch_shapes=[
            pltpu.VMEM((blocks, rows, width), jnp.bfloat16),
            pltpu.VMEM((blocks, rows, lanes), jnp.float32),
            pltpu.VMEM((factor, steps, length), jnp.float32),
        ],
        compiler_params=pltpu.CompilerParams(
            dimension_semantics=("arbitrary",), vmem_limit_bytes=VMEM_LIMIT
        ),
        cost_estimate=pl.CostEstimate(
            flops=steps * flops * 3,
            bytes_accessed=bias.size * 4 + 4 * length * width * steps,
            transcendentals=steps * heads * length * length,
        ),
        name="sequences",
    )(rank, *xs, bias, *weights)


def deal_kernel(chunks, rank_ref, x_ref, *out_refs):
    blocks = x_ref.shape[0]
    part = x_ref.shape[1] // chunks
    for c in range(chunks):
        for d in range(blocks):
            source = lax.rem(rank_ref[0] + d, blocks)
            out_refs[c * blocks + d][...] = x_ref[source, c * part : (c + 1) * part]


def collect_kernel(chunks, rank_ref, *refs):
    in_refs, (out_ref, left_ref) = refs[:-2], refs[-2:]
    blocks = out_ref.shape[0]
    part = out_ref.shape[1] // chunks
    lanes = left_ref.shape[3]
    for c in range(chunks):
        for d in range(blocks):
            target = lax.rem(rank_ref[0] + blocks - d, blocks)
            y_ref = in_refs[c * blocks + d]
            out_ref[target, c * part : (c + 1) * part] = y_ref[:part]
            left_ref[target, c] = y_ref[part, :, :lanes]


def vmem_call(kernel, shapes, rank, arrays, name):
    return pl.pallas_call(
        kernel,
        in_specs=[pl.BlockSpec(memory_space=pltpu.SMEM)]
        + [pl.BlockSpec(memory_space=pltpu.VMEM)] * len(arrays),
        out_specs=[pl.BlockSpec(memory_space=pltpu.VMEM)] * len(shapes),
        out_shape=[jax.ShapeDtypeStruct(a, jnp.bfloat16) for a in shapes],
        compiler_params=pltpu.CompilerParams(vmem_limit_bytes=VMEM_LIMIT // 2),
        cost_estimate=pl.CostEstimate(
            flops=0, bytes_accessed=4 * sum(a.size for a in arrays), transcendentals=0
        ),
        name=name,
    )(rank, *arrays)


def shift_all(arrays):
    size = len(arrays)
    return [arrays[0]] + [
        lax.ppermute(arrays[d], "res", [(r, (r + d) % size) for r in range(size)])
        for d in range(1, size)
    ]


def product_kernel(rows, seq_total, left_ref, *refs):
    right_refs, (table_ref, pair_ref, out_ref, stack) = refs[:-4], refs[-4:]
    groups, factor, part, cols = right_refs[0].shape
    scale = 1.0 / seq_total
    left = left_ref[...]
    for e in range(factor):
        right = jnp.concatenate(
            [ref[:, e].reshape(groups * part, cols) for ref in right_refs], axis=0
        )
        outer = (dot_f32(left, right, 1, 0) * scale).astype(jnp.bfloat16)
        stack[:, e * factor : (e + 1) * factor, :] = outer.reshape(rows, factor, cols)
    for i in range(rows):
        update = dot_f32(table_ref[...], stack[i], 1, 0)
        out_ref[i] = (pair_ref[i].astype(jnp.float32) + update.T).astype(jnp.bfloat16)


def run_product(left, rights, table, pair):
    total_rows, seq_total = left.shape
    _, factor, _, cols = rights[0].shape
    pair_rows = pair.shape[0]
    rows = math.gcd(pair_rows, 8)
    width = pair.shape[2]
    return pl.pallas_call(
        functools.partial(product_kernel, rows, seq_total),
        grid=(pair_rows // rows,),
        in_specs=[
            pl.BlockSpec((rows * factor, seq_total), lambda b: (b, 0)),
            *[
                pl.BlockSpec(a.shape, lambda b: (0, 0, 0, 0), pipeline_mode=pl.Buffered(1))
                for a in rights
            ],
            pl.BlockSpec(table.shape, lambda b: (0, 0), pipeline_mode=pl.Buffered(1)),
            pl.BlockSpec((rows, cols, width), lambda b: (b, 0, 0)),
        ],
        out_specs=pl.BlockSpec((rows, cols, width), lambda b: (b, 0, 0)),
        out_shape=jax.ShapeDtypeStruct(pair.shape, jnp.bfloat16),
        scratch_shapes=[pltpu.VMEM((rows, factor * factor, cols), jnp.bfloat16)],
        compiler_params=pltpu.CompilerParams(
            dimension_semantics=("arbitrary",), vmem_limit_bytes=VMEM_LIMIT
        ),
        cost_estimate=pl.CostEstimate(
            flops=4 * total_rows * cols * factor * (seq_total + width),
            bytes_accessed=2 * (left.size * (1 + cols * factor // total_rows) + left.size + 2 * pair.size),
            transcendentals=0,
        ),
        name="product",
    )(left, *rights, table, pair)


def permuted_on_device(
    aligned_activity,
    pair_state,
    focus_scaling_vector,
    combined_probe_matrix,
    sigmoid_offset_vector,
    focus_final_matrix,
    pair_norm_gain,
    pair_bias_matrix,
    feedforward_scaling_vector,
    feedforward_widen_matrix,
    feedforward_shrink_matrix,
    tensor_scaling_vector,
    twin_operand_matrix,
    tensor_final_matrix,
):
    width = aligned_activity.shape[2]
    heads = pair_bias_matrix.shape[1]
    factor = twin_operand_matrix.shape[1] // 2
    res_axis = lax.axis_size("res")
    seq_axis = lax.axis_size("seq")
    rows = aligned_activity.shape[1]
    seq_count = aligned_activity.shape[0] // res_axis
    length = rows * res_axis
    col_block = pair_state.shape[1]
    chunks = math.gcd(CHUNKS, seq_count)
    per_chunk = seq_count // chunks
    pack = per_chunk

    groups = math.gcd(GROUPS, chunks) if seq_count % (8 * GROUPS) == 0 else 1
    rank = lax.axis_index("res").astype(jnp.int32).reshape(1)
    pieces = aligned_activity.reshape(res_axis, seq_count, rows, width)
    dealt = vmem_call(
        functools.partial(deal_kernel, chunks),
        [(per_chunk, rows, width)] * (chunks * res_axis),
        rank,
        [pieces],
        "deal",
    )
    arrived = [shift_all(dealt[c * res_axis : (c + 1) * res_axis]) for c in range(chunks)]

    pair_norm = layer_normalize(pair_state.astype(jnp.float32), pair_norm_gain)
    bias_tile = jnp.einsum(
        "ijc,ch->hij", pair_norm, pair_bias_matrix, precision=lax.Precision.HIGHEST
    ).astype(jnp.bfloat16)
    bias_rows = lax.all_gather(bias_tile, "res", axis=1, tiled=True)
    bias_all = lax.all_gather(bias_rows, "seq", axis=0)
    bias = bias_all.transpose(1, 0, 3, 2).reshape(heads, length, length)
    bias = bias.astype(jnp.float32) * LOG2E

    left_w = twin_operand_matrix[:, :factor]
    left_w = jnp.stack(
        [jnp.pad(left_w, ((0, 0), (t * factor, (pack - 1 - t) * factor))) for t in range(pack)]
    )
    weights = (
        focus_scaling_vector.reshape(1, -1),
        combined_probe_matrix.T,
        sigmoid_offset_vector.reshape(-1, 1),
        focus_final_matrix,
        feedforward_scaling_vector.reshape(1, -1),
        feedforward_widen_matrix,
        feedforward_shrink_matrix,
        tensor_scaling_vector.reshape(1, -1),
        left_w,
        twin_operand_matrix[:, factor:].T,
    )
    returned, rights, pending = [], [], []
    for c in range(chunks):
        *updated, right = run_sequences(rank, arrived[c], bias, weights, heads, pack, seq_axis)
        returned += shift_all(updated)
        pending.append(right)
        if len(pending) == chunks // groups:
            right = jnp.concatenate(pending, axis=2)
            right = lax.all_to_all(right, "seq", split_axis=0, concat_axis=0, tiled=True)
            rights.append(lax.all_gather(right, "res", axis=0, tiled=True))
            pending = []
    if (seq_count // groups) % 8 != 0:
        rights = [r.transpose(1, 0, 2, 3).reshape(1, factor, -1, col_block) for r in rights]
    alignment_output, left = vmem_call(
        functools.partial(collect_kernel, chunks),
        [pieces.shape, (res_axis, chunks, rows, pack * factor)],
        rank,
        returned,
        "collect",
    )
    alignment_output = alignment_output.reshape(aligned_activity.shape)
    left = lax.all_gather(left, "seq", axis=0)
    left = left.reshape(seq_axis, res_axis, groups, chunks // groups, rows, pack, factor)
    left = left.transpose(4, 6, 2, 1, 0, 3, 5).reshape(rows * factor, -1)

    table = tensor_final_matrix.reshape(factor, factor, -1).transpose(2, 1, 0)
    table = table.reshape(table.shape[0], -1)
    pair_output = run_product(left, rights, table, pair_state)
    return (alignment_output, pair_output)


MESH = pl.DeviceIdType.MESH
GROUP = 8
AHEAD = 8
FIRST = 2
FILL = 0
UNROLL = 8
SLOW = 2
FAST = 11
LANES = 128


def dot_t(a, b):
    return dot_f32(a, b, 1, 1)


def split3(values):
    first = values.astype(jnp.bfloat16)
    rest = values - first.astype(jnp.float32)
    second = rest.astype(jnp.bfloat16)
    third = (rest - second.astype(jnp.float32)).astype(jnp.bfloat16)
    return jnp.concatenate([first, second, third], axis=0)


def wait_for(ref, sem):
    pltpu.make_async_copy(ref, ref, sem).wait()


def send(src, dst, sent, arrived, **peer):
    pltpu.make_async_remote_copy(
        src_ref=src,
        dst_ref=dst,
        send_sem=sent,
        recv_sem=arrived,
        device_id=peer,
        device_id_type=MESH,
    ).start()


class Relay:
    def __init__(self, rank, deep, wide, tile, tiles, arrived, sent_z, sent_x, forward=None):
        self.rank, self.deep, self.wide = rank, deep, wide
        self.z, self.x = rank // wide, rank % wide
        self.tile, self.tiles, self.arrived = tile, tiles, arrived
        self.sent_z, self.sent_x, self.forward = sent_z, sent_x, forward

    def pass_on(self, owner):
        for d in range(1, self.wide):
            peer = self.z * self.wide + (self.x + d) % self.wide
            send(self.tile(owner), self.tile(owner), self.sent_x, self.arrived.at[owner], res=peer)
        if self.forward is not None:
            self.forward(owner)

    def ends(self, hop, way):
        z = self.z - hop if way == 0 else self.z + hop
        there = z >= 0 if way == 0 else z < self.deep
        onward = self.z + 1 < self.deep if way == 0 else self.z >= 1
        peer = self.rank + self.wide if way == 0 else self.rank - self.wide
        return z * self.wide + self.x, there, onward, peer

    def start(self):
        for way in range(2):
            owner, _, onward, peer = self.ends(0, way)

            @pl.when(onward)
            def _():
                send(
                    self.tile(self.rank),
                    self.tile(self.rank),
                    self.sent_z.at[0, way],
                    self.arrived.at[self.rank],
                    res=peer,
                )

        self.pass_on(self.rank)

    def hop(self, hop):
        for way in range(2):
            owner, there, onward, peer = self.ends(hop, way)

            @pl.when(there)
            def _():
                wait_for(self.tile(owner), self.arrived.at[owner])

                @pl.when(onward)
                def _():
                    send(
                        self.tile(owner),
                        self.tile(owner),
                        self.sent_z.at[hop, way],
                        self.arrived.at[owner],
                        res=peer,
                    )

                self.pass_on(owner)

    def across(self):
        for d in range(1, self.wide):
            for z in range(self.deep):
                owner = z * self.wide + (self.x + d) % self.wide
                wait_for(self.tile(owner), self.arrived.at[owner])
                if self.forward is not None:
                    self.forward(owner)

    def finish(self):
        for hop in range(self.deep):
            for way in range(2):
                owner, there, onward, _ = self.ends(hop, way)

                @pl.when(jnp.logical_and(there, onward))
                def _():
                    wait_for(self.tile(owner), self.sent_z.at[hop, way])

        for d in range(1, self.wide):
            wait_for(self.tiles(self.deep), self.sent_x)


def fused_kernel(heads, ranks, wide, x_ref, pair_ref, *refs):
    given, refs = refs[:12], refs[12:]
    (out_ref, pair_out_ref), refs = refs[:2], refs[2:]
    held, refs = refs[:12], refs[12:]
    (
        gain_ref,
        probe_rows,
        offset_row,
        final_ref,
        ff_gain_ref,
        widen_ref,
        shrink_ref,
        opm_gain_ref,
        twin_ref,
        pair_gain_ref,
        pair_w_ref,
        table_rows,
    ) = held
    (
        xbuf,
        pairv,
        early,
        tile_s,
        tiles,
        bias,
        acc,
        left_acc,
        stage,
        right_v,
        left_out,
        left_in,
        left_s,
        left_t,
        normal,
        left_v,
        stack,
        probe_ref,
        offset_ref,
        table_s,
        table_ref,
    ), sems = refs[:21], refs[21:]
    (
        pair_sem,
        held_sem,
        x_in,
        x_out,
        ret_in,
        ret_out,
        tile_in,
        tile_z,
        tile_x,
        twin_out,
        twin_in,
        right_in,
        right_z,
        right_x,
        half_out,
        half_in,
        half_own,
        left_sem,
    ) = sems
    rank = lax.axis_index("res")
    core = lax.axis_index("seq")
    blocks, steps, rows, width = xbuf.shape
    length = blocks * rows
    depth = width // heads
    factor = twin_ref.shape[0] // 2
    cols = length // 2
    spans = steps // GROUP
    deep = ranks // wide

    barrier = pltpu.get_barrier_semaphore()
    for d in range(1, blocks):
        pl.semaphore_signal(
            barrier, inc=1, device_id={"res": (rank + d) % blocks}, device_id_type=MESH
        )
    pl.semaphore_signal(barrier, inc=1, device_id={"seq": 1 - core}, device_id_type=MESH)
    pair_copy = pltpu.make_async_copy(pair_ref, pairv, pair_sem.at[0])
    pair_copy.start()
    copies = [
        pltpu.make_async_copy(given[i], held[i], held_sem.at[i]) for i in range(len(given))
    ]
    for copy in copies:
        copy.start()
    pl.semaphore_wait(barrier, blocks)

    def send_x(s):
        for d in range(1, blocks):
            to = (rank + d) % blocks
            send(x_ref.at[to * steps + s], xbuf.at[rank, s], x_out.at[0], x_in.at[s], res=to)
        pltpu.make_async_copy(x_ref.at[rank * steps + s], xbuf.at[rank, s], x_in.at[s]).start()

    def send_back(s):
        def all_to(target, arrived):
            for d in range(1, blocks):
                to = (rank + d) % blocks
                send(xbuf.at[to, s], target, ret_out.at[0], arrived, res=to)
            pltpu.make_async_copy(xbuf.at[rank, s], target, arrived).start()

        @pl.when(s < GROUP)
        def _():
            all_to(early.at[rank, s], ret_in.at[0])

        @pl.when(s >= GROUP)
        def _():
            all_to(out_ref.at[rank * steps + s], ret_in.at[1])

    for s in range(FIRST):
        send_x(s)
    for copy in copies:
        copy.wait()
    pair_copy.wait()

    scaled = split3(pair_w_ref[...])

    def tile_rows(i, carry):
        normed = split3(layer_normalize(pairv[i].astype(jnp.float32), pair_gain_ref[...]))
        parts = dot_t(scaled, normed)
        tile = jnp.zeros((heads, cols), jnp.float32)
        for a, b in ((2, 0), (1, 1), (0, 2), (1, 0), (0, 1), (0, 0)):
            tile = tile + parts[a * heads : (a + 1) * heads, b * cols : (b + 1) * cols]
        for h in range(heads):
            tile_s[h, pl.ds(i, 1), :] = tile[h : h + 1]
        return carry

    lax.fori_loop(0, rows, tile_rows, 0, unroll=UNROLL)
    pack = LANES // rows
    for p in range(heads // pack):
        both = tile_s[p * pack : (p + 1) * pack].reshape(LANES, cols)
        tiles[core, rank, p] = both.T.astype(jnp.bfloat16)

    def to_twin(owner):
        send(
            tiles.at[core, owner], tiles.at[core, owner], twin_out.at[0], twin_in.at[0], seq=1 - core
        )

    spread = Relay(
        rank,
        deep,
        wide,
        lambda o: tiles.at[core, o],
        lambda c: tiles.at[core, pl.ds(0, c)],
        tile_in,
        tile_z,
        tile_x.at[0],
        to_twin,
    )

    def prepare():
        for c in range(0, probe_rows.shape[1], width):
            columns = probe_rows[:, c : c + width].astype(jnp.float32)
            probe_ref[c : c + width] = columns.T.astype(jnp.bfloat16)
        offset_ref[...] = jnp.broadcast_to(offset_row[...], (LANES, width)).T
        table_s[...] = table_rows[...].astype(jnp.float32)
        few = LANES // factor
        for e in range(0, factor, few):
            lines = [table_s[pl.ds(e + i, factor, stride=factor), :] for i in range(few)]
            lines = jnp.concatenate(lines, axis=0)
            table_ref[:, e * factor : (e + few) * factor] = lines.T.astype(jnp.bfloat16)

    spread.start()
    send_x(FIRST)
    prepare()
    for hop in range(1, deep):
        spread.hop(hop)
        if FIRST + hop < AHEAD:
            send_x(FIRST + hop)
    for s in range(min(FIRST + deep, AHEAD), AHEAD):
        send_x(s)
    spread.across()
    wait_for(tiles.at[1 - core], twin_in.at[0])

    low = lax.broadcasted_iota(jnp.int32, (cols, LANES), 1) < rows

    def fill(step, carry):
        half, p = step // (heads // pack), step % (heads // pack)
        for k in range(blocks // pack):
            even = tiles[half, pack * k, p].astype(jnp.float32) * LOG2E
            odd = tiles[half, pack * k + 1, p].astype(jnp.float32) * LOG2E
            here = (pl.ds(pl.multiple_of(half * cols, cols), cols), slice(k * LANES, (k + 1) * LANES))
            bias[(pack * p,) + here] = jnp.where(low, even, pltpu.roll(odd, rows, 1))
            bias[(pack * p + 1,) + here] = jnp.where(low, pltpu.roll(even, rows, 1), odd)
        return carry

    lax.fori_loop(0, 2 * heads // pack, fill, 0)

    def relay_of(u):
        return Relay(
            rank,
            deep,
            wide,
            lambda o: right_v.at[:, u, o],
            lambda c: right_v.at[:, u, pl.ds(0, c)],
            right_in.at[u],
            right_z.at[u],
            right_x.at[u],
        )

    def swap_halves(u):
        send(stage.at[u, 1], right_v.at[core, u, rank], half_out.at[u], half_in.at[u], seq=1 - core)
        pltpu.make_async_copy(stage.at[u, 0], right_v.at[core, u, rank], half_own.at[u]).start()

    def start_right(u):
        wait_for(right_v.at[core, u, rank], half_own.at[u])
        wait_for(right_v.at[1 - core, u, rank], half_in.at[u])
        relay_of(u).start()

    def due(s):
        early = steps - AHEAD
        slow = early * SLOW // 10
        return jnp.where(s <= early, s * SLOW // 10, slow + (s - early) * FAST // 10)

    def send_back_upto(first, end):
        def one(s, carry):
            send_back(s)
            return carry

        lax.fori_loop(first, end, one, 0)

    ones = jnp.ones((16, length), jnp.bfloat16)

    def sequence(s, carry):
        wait_for(xbuf.at[:, s], x_in.at[s])

        @pl.when(s + AHEAD < steps)
        def _():
            send_x(s + AHEAD)

        u, place = s // GROUP - 1, s % GROUP

        @pl.when(jnp.logical_and(u >= 0, place == 0))
        def _():
            swap_halves(u)

        send_back_upto(due(s), due(s + 1))

        @pl.when(jnp.logical_and(u >= 0, place == 1))
        def _():
            start_right(u)

        @pl.when(jnp.logical_and(u >= 0, jnp.logical_and(place > 1, place % 2 == 1)))
        def _():
            relay_of(u).hop(place // 2)

        x = xbuf[:, s].astype(jnp.float32).reshape(length, width)
        normed = layer_normalize(x, gain_ref[...]).astype(jnp.bfloat16)
        mapped = dot_t(probe_ref[...], normed)
        q = (mapped[:width] * (depth ** (-0.5) * LOG2E)).astype(jnp.bfloat16)
        k = mapped[width : 2 * width].astype(jnp.bfloat16)
        v = mapped[2 * width : 3 * width].astype(jnp.bfloat16)
        gate = jax.nn.sigmoid(mapped[3 * width :] + offset_ref[:, :1])
        gated = []
        for h in range(heads):
            part = slice(h * depth, (h + 1) * depth)
            scores = dot_f32(k[part], q[part], 0, 0) + bias[h]
            top = jnp.max(scores, axis=0, keepdims=True)
            p = jnp.exp2(scores - top).astype(jnp.bfloat16)
            mixed = dot_f32(jnp.concatenate([v[part], ones], axis=0), p, 1, 0)
            share = mixed[:depth] / mixed[depth : depth + 1]
            gated.append((share * gate[part]).astype(jnp.bfloat16))
        gated = jnp.concatenate(gated, axis=0)
        stream = x + dot_f32(gated, final_ref[...], 0, 0)
        normed = layer_normalize(stream, ff_gain_ref[...]).astype(jnp.bfloat16)
        hidden = jnp.maximum(dot_f32(normed, widen_ref[...], 1, 0), 0.0).astype(jnp.bfloat16)
        stream = stream + dot_f32(hidden, shrink_ref[...], 1, 0)
        updated = stream.astype(jnp.bfloat16)
        xbuf[:, s] = stream.reshape(blocks, rows, width).astype(jnp.bfloat16)
        normed = layer_normalize(updated.astype(jnp.float32), opm_gain_ref[...]).astype(jnp.bfloat16)
        factors = dot_t(twin_ref[...], normed)
        for e in range(factor):
            left_acc[e, pl.ds(place, 1), :] = factors[e : e + 1]
            acc[e, pl.ds(place, 1), :] = factors[factor + e : factor + e + 1]

        @pl.when(place == GROUP - 1)
        def _():
            own = pl.ds(pl.multiple_of(core * cols, cols), cols)
            other = pl.ds(pl.multiple_of((1 - core) * cols, cols), cols)
            stage[u + 1, 0] = acc[:, :, own].astype(jnp.bfloat16)
            stage[u + 1, 1] = acc[:, :, other].astype(jnp.bfloat16)

        return carry

    lax.fori_loop(0, steps, sequence, 0)

    last = spans - 1
    sent = due(steps)
    swap_halves(last)
    pairs = factor // 2
    near = lax.broadcasted_iota(jnp.int32, (pairs, GROUP, LANES), 2) < rows
    for m in range(blocks // 2):
        lanes = slice(m * LANES, (m + 1) * LANES)
        one, two = left_acc[:pairs, :, lanes], left_acc[pairs:, :, lanes]
        left_out[2 * m] = jnp.where(near, one, pltpu.roll(two, rows, 2)).astype(jnp.bfloat16)
        left_out[2 * m + 1] = jnp.where(near, pltpu.roll(one, rows, 2), two).astype(jnp.bfloat16)
    start_right(last)
    for d in range(1, blocks):
        to = (rank + d) % blocks
        send(left_out.at[to], left_in.at[rank], left_sem.at[0], left_sem.at[1], res=to)
    pltpu.make_async_copy(left_out.at[rank], left_in.at[rank], left_sem.at[1]).start()

    def normalize(b, carry):
        values = early[b].astype(jnp.float32).reshape(-1, width)
        values = layer_normalize(values, opm_gain_ref[...]).astype(jnp.bfloat16)
        place = pl.ds(pl.multiple_of(b * GROUP * rows, GROUP * rows), GROUP * rows)
        for c in range(width // LANES):
            lanes = values[:, c * LANES : (c + 1) * LANES]
            normal[c, place, :] = lanes.astype(jnp.float32)
        return carry

    def left_rows(i, carry):
        values = [
            normal[c, pl.ds(i, blocks * GROUP, stride=rows), :].astype(jnp.bfloat16)
            for c in range(width // LANES)
        ]
        values = dot_t(twin_ref[:factor], jnp.concatenate(values, axis=1))
        left_s[pl.ds(pl.multiple_of(i * factor, factor), factor), : LANES // 2] = values
        return carry

    def early_left():
        wait_for(early, ret_in.at[0])
        for b in range(blocks):
            target = out_ref.at[pl.ds(b * steps, GROUP)]
            pltpu.make_async_copy(early.at[b], target, ret_in.at[2]).start()
        lax.fori_loop(0, blocks, normalize, 0)
        lax.fori_loop(0, rows, left_rows, 0, unroll=8)

    for hop in range(1, deep):
        relay_of(last).hop(hop)
        send_back_upto(sent + (hop - 1) * FILL, sent + hop * FILL)
    send_back_upto(sent + (deep - 1) * FILL, steps)
    early_left()

    wait_for(left_in, left_sem.at[1])
    for c in range(pairs):
        values = left_in[:, c].astype(jnp.float32).reshape(blocks * GROUP, LANES).T
        values = jnp.concatenate([values, values], axis=1)
        for half in range(2):
            part = values[half * rows : (half + 1) * rows]
            left_t[pl.ds(half * pairs + c, rows, stride=factor), :] = part
    first = lax.broadcasted_iota(jnp.int32, left_s.shape, 1) < LANES // 2
    left_v[core] = jnp.where(first, left_s[...], left_t[...]).astype(jnp.bfloat16)
    send(left_v.at[core], left_v.at[core], left_sem.at[2], left_sem.at[3], seq=1 - core)
    for u in range(spans):
        relay_of(u).across()
    wait_for(left_v.at[1 - core], left_sem.at[3])

    some = stack.shape[0]
    scale = 1.0 / (2 * blocks * steps)

    def pair_block(b, carry):
        place = pl.ds(pl.multiple_of(b * some * factor, some * factor), some * factor)
        left = jnp.concatenate([left_v[0, place, :], left_v[1, place, :]], axis=1)
        for e in range(factor):
            right = right_v[:, :, :, e].reshape(2 * blocks * steps, cols)
            outer = (dot_f32(left, right, 1, 0) * scale).astype(jnp.bfloat16)
            stack[:, e * factor : (e + 1) * factor, :] = outer.reshape(some, factor, cols)
        for i in range(some):
            update = dot_f32(table_ref[...], stack[i], 1, 0)
            at = b * some + i
            pairv[at] = (pairv[at].astype(jnp.float32) + update.T).astype(jnp.bfloat16)
        these = pl.ds(b * some, some)
        pltpu.make_async_copy(pairv.at[these], pair_out_ref.at[these], pair_sem.at[1]).start()
        return carry

    lax.fori_loop(0, rows // some, pair_block, 0)

    wait_for(x_ref.at[pl.ds(0, (blocks - 1) * steps)], x_out.at[0])
    wait_for(out_ref.at[pl.ds(0, (blocks - 1) * steps)], ret_out.at[0])
    spread.finish()
    wait_for(tiles.at[core], twin_out.at[0])
    for u in range(spans):
        relay_of(u).finish()
        wait_for(stage.at[u, 1], half_out.at[u])
    wait_for(left_out.at[pl.ds(0, blocks - 1)], left_sem.at[0])
    wait_for(left_v.at[core], left_sem.at[2])
    wait_for(out_ref.at[pl.ds(0, blocks * (steps - GROUP))], ret_in.at[1])
    wait_for(early, ret_in.at[2])
    wait_for(pairv, pair_sem.at[1])


def run_fused(x, pair, weights, heads, ranks, wide):
    sequences, rows, width = x.shape
    steps = sequences // ranks
    length = rows * ranks
    cols = pair.shape[1]
    factor = weights[8].shape[0] // 2
    spans = steps // GROUP
    deep = ranks // wide
    pack = LANES // rows
    table = weights[11].shape
    any_spec = pl.BlockSpec(memory_space=pl.ANY)
    dma = lambda *shape: pltpu.SemaphoreType.DMA(shape)
    half = lambda *shape: pltpu.VMEM(shape, jnp.bfloat16)
    full = lambda *shape: pltpu.VMEM(shape, jnp.float32)
    return pl.pallas_call(
        functools.partial(fused_kernel, heads, ranks, wide),
        in_specs=[any_spec] * (2 + len(weights)),
        out_specs=[any_spec] * 2,
        out_shape=[jax.ShapeDtypeStruct(a, jnp.bfloat16) for a in (x.shape, pair.shape)],
        scratch_shapes=[pltpu.VMEM(a.shape, a.dtype) for a in weights]
        + [
            half(ranks, steps, rows, width),
            half(*pair.shape),
            half(ranks, GROUP, rows, width),
            full(heads, rows, cols),
            half(2, ranks, heads // pack, cols, LANES),
            full(heads, length, length),
            full(factor, GROUP, length),
            full(factor, GROUP, length),
            half(spans, 2, factor, GROUP, cols),
            half(2, spans, ranks, factor, GROUP, cols),
            half(ranks, factor // 2, GROUP, LANES),
            half(ranks, factor // 2, GROUP, LANES),
            full(rows * factor, LANES),
            full(rows * factor, LANES),
            full(width // LANES, ranks * GROUP * rows, LANES),
            half(2, rows * factor, LANES),
            half(math.gcd(rows, 8), factor * factor, cols),
            half(4 * width, width),
            full(width, LANES),
            full(*table),
            half(table[1], table[0]),
            dma(2),
            dma(len(weights)),
            dma(steps),
            dma(1),
            dma(3),
            dma(1),
            dma(ranks),
            dma(deep, 2),
            dma(1),
            dma(1),
            dma(1),
            dma(spans, ranks),
            dma(spans, deep, 2),
            dma(spans),
            dma(spans),
            dma(spans),
            dma(spans),
            dma(4),
        ],
        compiler_params=pltpu.CompilerParams(
            vmem_limit_bytes=FUSED_VMEM, collective_id=0, has_side_effects=True
        ),
        name="fused",
    )(x, pair, *weights)


def fits(rows, steps, ranks, heads, channels, seq_axis):
    return (
        seq_axis == 2
        and rows * 2 == LANES
        and heads == 8
        and channels == LANES
        and ranks % 2 == 0
        and steps == 2 * GROUP
        and ranks == GROUP
        and steps >= AHEAD
    )


def fused_on_device(
    aligned_activity,
    pair_state,
    focus_scaling_vector,
    combined_probe_matrix,
    sigmoid_offset_vector,
    focus_final_matrix,
    pair_norm_gain,
    pair_bias_matrix,
    feedforward_scaling_vector,
    feedforward_widen_matrix,
    feedforward_shrink_matrix,
    tensor_scaling_vector,
    twin_operand_matrix,
    tensor_final_matrix,
):
    heads = pair_bias_matrix.shape[1]
    weights = (
        focus_scaling_vector.reshape(1, -1),
        combined_probe_matrix,
        sigmoid_offset_vector.reshape(1, -1),
        focus_final_matrix,
        feedforward_scaling_vector.reshape(1, -1),
        feedforward_widen_matrix,
        feedforward_shrink_matrix,
        tensor_scaling_vector.reshape(1, -1),
        twin_operand_matrix.T,
        pair_norm_gain.reshape(1, -1),
        pair_bias_matrix.T,
        tensor_final_matrix,
    )
    return tuple(
        run_fused(aligned_activity, pair_state, weights, heads, lax.axis_size("res"), 2)
    )


def on_device(aligned_activity, pair_state, *parameters):
    ranks = lax.axis_size("res")
    rows = aligned_activity.shape[1]
    steps = aligned_activity.shape[0] // ranks
    heads = parameters[5].shape[1]
    if fits(rows, steps, ranks, heads, pair_state.shape[2], lax.axis_size("seq")):
        return fused_on_device(aligned_activity, pair_state, *parameters)
    return permuted_on_device(aligned_activity, pair_state, *parameters)


def solution(mesh):
    return jax.shard_map(
        on_device,
        mesh=mesh,
        in_specs=(
            P(("grp", "seq"), "res", None),
            P(("grp", "res"), "seq", None),
            P(),
            P(),
            P(),
            P(),
            P(),
            P(),
            P(),
            P(),
            P(),
            P(),
            P(),
            P(),
        ),
        out_specs=(P(("grp", "seq"), "res", None), P(("grp", "res"), "seq", None)),
        check_vma=False,
    )
```

```python
import functools
import math

import jax
import jax.numpy as jnp
from jax import lax
from jax.experimental import pallas as pl
from jax.experimental.pallas import tpu as pltpu
from jax.sharding import PartitionSpec as P

LOG2E = math.log2(math.e)
VMEM_LIMIT = 60 * 1024 * 1024
FUSED_VMEM = 54 * 1024 * 1024
CHUNKS = 4
GROUPS = 2


def layer_normalize(inputs, scale_gain):
    sample_expectation = jnp.mean(inputs, axis=-1, keepdims=True)
    centered = inputs - sample_expectation
    variance = jnp.mean(centered * centered, axis=-1, keepdims=True)
    return centered * lax.rsqrt(variance + 1e-05) * scale_gain


def dot_f32(a, b, ca, cb):
    return lax.dot_general(a, b, (((ca,), (cb,)), ((), ())), preferred_element_type=jnp.float32)


def sequence_kernel(
    heads,
    pack,
    blocks,
    *refs,
):
    rank_ref, refs = refs[0], refs[1:]
    x_refs, refs = refs[:blocks], refs[blocks:]
    weight_refs, refs = refs[:11], refs[11:]
    out_refs, (right_ref, gathered, left_acc, right_acc) = refs[:blocks], refs[blocks:]
    (
        bias_ref,
        gain_ref,
        probe_ref,
        offset_ref,
        final_ref,
        ff_gain_ref,
        widen_ref,
        shrink_ref,
        opm_gain_ref,
        left_w_ref,
        right_w_ref,
    ) = weight_refs
    rank = rank_ref[0]
    step = pl.program_id(0)
    steps = right_ref.shape[2]
    _, rows, width = x_refs[0].shape
    length = blocks * rows
    depth = width // heads
    for d in range(blocks):
        gathered[lax.rem(rank + blocks - d, blocks)] = x_refs[d][0]
    x = gathered[...].astype(jnp.float32).reshape(length, width)
    normed = layer_normalize(x, gain_ref[...]).astype(jnp.bfloat16)
    mapped = dot_f32(probe_ref[...], normed, 1, 1)
    q = (mapped[:width] * (depth ** (-0.5) * LOG2E)).astype(jnp.bfloat16)
    k = mapped[width : 2 * width].astype(jnp.bfloat16)
    v = mapped[2 * width : 3 * width].astype(jnp.bfloat16)
    gate = jax.nn.sigmoid(mapped[3 * width :] + offset_ref[...])
    def due(s):
        early = steps - AHEAD
        slow = early * SLOW // 10
        return jnp.where(s <= early, s * SLOW // 10, slow + (s - early) * FAST // 10)

    def send_back_upto(first, end):
        def one(s, carry):
            send_back(s)
            return carry

        lax.fori_loop(first, end, one, 0)

    ones = jnp.ones((16, length), jnp.bfloat16)
    gated = []
    for h in range(heads):
        part = slice(h * depth, (h + 1) * depth)
        scores = dot_f32(k[part], q[part], 0, 0) + bias_ref[h]
        top = jnp.max(scores, axis=0, keepdims=True)
        p = jnp.exp2(scores - top).astype(jnp.bfloat16)
        mixed = dot_f32(jnp.concatenate([v[part], ones], axis=0), p, 1, 0)
        share = mixed[:depth] / mixed[depth : depth + 1]
        gated.append((share * gate[part]).astype(jnp.bfloat16))
    gated = jnp.concatenate(gated, axis=0)
    stream = x + dot_f32(gated, final_ref[...], 0, 0)
    normed = layer_normalize(stream, ff_gain_ref[...]).astype(jnp.bfloat16)
    hidden = jnp.maximum(dot_f32(normed, widen_ref[...], 1, 0), 0.0).astype(jnp.bfloat16)
    stream = stream + dot_f32(hidden, shrink_ref[...], 1, 0)
    updated = stream.astype(jnp.bfloat16)
    gathered[...] = stream.reshape(blocks, rows, width).astype(jnp.bfloat16)
    for d in range(blocks):
        out_refs[d][step] = gathered[lax.rem(rank + d, blocks)]
    normed = layer_normalize(updated.astype(jnp.float32), opm_gain_ref[...]).astype(jnp.bfloat16)
    slot = lax.rem(step, pack)
    left = dot_f32(normed, left_w_ref[slot], 1, 0).reshape(left_acc.shape)

    @pl.when(slot == 0)
    def _():
        left_acc[...] = left

    @pl.when(slot != 0)
    def _():
        left_acc[...] = left_acc[...] + left

    factor = right_w_ref.shape[0]
    right = dot_f32(right_w_ref[...], normed, 1, 1)
    for e in range(factor):
        right_acc[e, pl.ds(step, 1), :] = right[e : e + 1]

    @pl.when(step == steps - 1)
    def _():
        lanes = left_acc.shape[2]
        cols = right_ref.shape[3]
        for part in range(right_ref.shape[0]):
            right_ref[part] = right_acc[:, :, part * cols : (part + 1) * cols].astype(jnp.bfloat16)
        for d in range(blocks):
            if lanes < width:
                out_refs[d][steps] = jnp.zeros((rows, width), jnp.bfloat16)
            out_refs[d][steps, :, :lanes] = left_acc[lax.rem(rank + d, blocks)].astype(jnp.bfloat16)


def run_sequences(rank, xs, bias, weights, heads, pack, halves):
    blocks = len(xs)
    steps, rows, width = xs[0].shape
    length = blocks * rows
    factor = weights[-1].shape[0]
    cols = length // halves
    whole = lambda a: pl.BlockSpec(
        a.shape, lambda s, n=a.ndim: (0,) * n, pipeline_mode=pl.Buffered(1)
    )
    kept = lambda shape: pl.BlockSpec(shape, lambda s, n=len(shape): (0,) * n)
    lanes = pack * factor
    hidden = weights[5].shape[1]
    flops = 2 * length * width * (5 * width + 2 * hidden + 128) + 4 * length * length * width
    shapes = [(steps + 1, rows, width)] * blocks + [(halves, factor, steps, cols)]
    return pl.pallas_call(
        functools.partial(sequence_kernel, heads, pack, blocks),
        grid=(steps,),
        in_specs=[pl.BlockSpec(memory_space=pltpu.SMEM)]
        + [pl.BlockSpec((1, rows, width), lambda s: (s, 0, 0)) for _ in xs]
        + [whole(a) for a in (bias,) + weights],
        out_specs=[kept(a) for a in shapes],
        out_shape=[jax.ShapeDtypeStruct(a, jnp.bfloat16) for a in shapes],
        scratch_shapes=[
            pltpu.VMEM((blocks, rows, width), jnp.bfloat16),
            pltpu.VMEM((blocks, rows, lanes), jnp.float32),
            pltpu.VMEM((factor, steps, length), jnp.float32),
        ],
        compiler_params=pltpu.CompilerParams(
            dimension_semantics=("arbitrary",), vmem_limit_bytes=VMEM_LIMIT
        ),
        cost_estimate=pl.CostEstimate(
            flops=steps * flops * 3,
            bytes_accessed=bias.size * 4 + 4 * length * width * steps,
            transcendentals=steps * heads * length * length,
        ),
        name="sequences",
    )(rank, *xs, bias, *weights)


def deal_kernel(chunks, rank_ref, x_ref, *out_refs):
    blocks = x_ref.shape[0]
    part = x_ref.shape[1] // chunks
    for c in range(chunks):
        for d in range(blocks):
            source = lax.rem(rank_ref[0] + d, blocks)
            out_refs[c * blocks + d][...] = x_ref[source, c * part : (c + 1) * part]


def collect_kernel(chunks, rank_ref, *refs):
    in_refs, (out_ref, left_ref) = refs[:-2], refs[-2:]
    blocks = out_ref.shape[0]
    part = out_ref.shape[1] // chunks
    lanes = left_ref.shape[3]
    for c in range(chunks):
        for d in range(blocks):
            target = lax.rem(rank_ref[0] + blocks - d, blocks)
            y_ref = in_refs[c * blocks + d]
            out_ref[target, c * part : (c + 1) * part] = y_ref[:part]
            left_ref[target, c] = y_ref[part, :, :lanes]


def vmem_call(kernel, shapes, rank, arrays, name):
    return pl.pallas_call(
        kernel,
        in_specs=[pl.BlockSpec(memory_space=pltpu.SMEM)]
        + [pl.BlockSpec(memory_space=pltpu.VMEM)] * len(arrays),
        out_specs=[pl.BlockSpec(memory_space=pltpu.VMEM)] * len(shapes),
        out_shape=[jax.ShapeDtypeStruct(a, jnp.bfloat16) for a in shapes],
        compiler_params=pltpu.CompilerParams(vmem_limit_bytes=VMEM_LIMIT // 2),
        cost_estimate=pl.CostEstimate(
            flops=0, bytes_accessed=4 * sum(a.size for a in arrays), transcendentals=0
        ),
        name=name,
    )(rank, *arrays)


def shift_all(arrays):
    size = len(arrays)
    return [arrays[0]] + [
        lax.ppermute(arrays[d], "res", [(r, (r + d) % size) for r in range(size)])
        for d in range(1, size)
    ]


def product_kernel(rows, seq_total, left_ref, *refs):
    right_refs, (table_ref, pair_ref, out_ref, stack) = refs[:-4], refs[-4:]
    groups, factor, part, cols = right_refs[0].shape
    scale = 1.0 / seq_total
    left = left_ref[...]
    for e in range(factor):
        right = jnp.concatenate(
            [ref[:, e].reshape(groups * part, cols) for ref in right_refs], axis=0
        )
        outer = (dot_f32(left, right, 1, 0) * scale).astype(jnp.bfloat16)
        stack[:, e * factor : (e + 1) * factor, :] = outer.reshape(rows, factor, cols)
    for i in range(rows):
        update = dot_f32(table_ref[...], stack[i], 1, 0)
        out_ref[i] = (pair_ref[i].astype(jnp.float32) + update.T).astype(jnp.bfloat16)


def run_product(left, rights, table, pair):
    total_rows, seq_total = left.shape
    _, factor, _, cols = rights[0].shape
    pair_rows = pair.shape[0]
    rows = math.gcd(pair_rows, 8)
    width = pair.shape[2]
    return pl.pallas_call(
        functools.partial(product_kernel, rows, seq_total),
        grid=(pair_rows // rows,),
        in_specs=[
            pl.BlockSpec((rows * factor, seq_total), lambda b: (b, 0)),
            *[
                pl.BlockSpec(a.shape, lambda b: (0, 0, 0, 0), pipeline_mode=pl.Buffered(1))
                for a in rights
            ],
            pl.BlockSpec(table.shape, lambda b: (0, 0), pipeline_mode=pl.Buffered(1)),
            pl.BlockSpec((rows, cols, width), lambda b: (b, 0, 0)),
        ],
        out_specs=pl.BlockSpec((rows, cols, width), lambda b: (b, 0, 0)),
        out_shape=jax.ShapeDtypeStruct(pair.shape, jnp.bfloat16),
        scratch_shapes=[pltpu.VMEM((rows, factor * factor, cols), jnp.bfloat16)],
        compiler_params=pltpu.CompilerParams(
            dimension_semantics=("arbitrary",), vmem_limit_bytes=VMEM_LIMIT
        ),
        cost_estimate=pl.CostEstimate(
            flops=4 * total_rows * cols * factor * (seq_total + width),
            bytes_accessed=2 * (left.size * (1 + cols * factor // total_rows) + left.size + 2 * pair.size),
            transcendentals=0,
        ),
        name="product",
    )(left, *rights, table, pair)


def permuted_on_device(
    aligned_activity,
    pair_state,
    focus_scaling_vector,
    combined_probe_matrix,
    sigmoid_offset_vector,
    focus_final_matrix,
    pair_norm_gain,
    pair_bias_matrix,
    feedforward_scaling_vector,
    feedforward_widen_matrix,
    feedforward_shrink_matrix,
    tensor_scaling_vector,
    twin_operand_matrix,
    tensor_final_matrix,
):
    width = aligned_activity.shape[2]
    heads = pair_bias_matrix.shape[1]
    factor = twin_operand_matrix.shape[1] // 2
    res_axis = lax.axis_size("res")
    seq_axis = lax.axis_size("seq")
    rows = aligned_activity.shape[1]
    seq_count = aligned_activity.shape[0] // res_axis
    length = rows * res_axis
    col_block = pair_state.shape[1]
    chunks = math.gcd(CHUNKS, seq_count)
    per_chunk = seq_count // chunks
    pack = per_chunk

    groups = math.gcd(GROUPS, chunks) if seq_count % (8 * GROUPS) == 0 else 1
    rank = lax.axis_index("res").astype(jnp.int32).reshape(1)
    pieces = aligned_activity.reshape(res_axis, seq_count, rows, width)
    dealt = vmem_call(
        functools.partial(deal_kernel, chunks),
        [(per_chunk, rows, width)] * (chunks * res_axis),
        rank,
        [pieces],
        "deal",
    )
    arrived = [shift_all(dealt[c * res_axis : (c + 1) * res_axis]) for c in range(chunks)]

    pair_norm = layer_normalize(pair_state.astype(jnp.float32), pair_norm_gain)
    bias_tile = jnp.einsum(
        "ijc,ch->hij", pair_norm, pair_bias_matrix, precision=lax.Precision.HIGHEST
    ).astype(jnp.bfloat16)
    bias_rows = lax.all_gather(bias_tile, "res", axis=1, tiled=True)
    bias_all = lax.all_gather(bias_rows, "seq", axis=0)
    bias = bias_all.transpose(1, 0, 3, 2).reshape(heads, length, length)
    bias = bias.astype(jnp.float32) * LOG2E

    left_w = twin_operand_matrix[:, :factor]
    left_w = jnp.stack(
        [jnp.pad(left_w, ((0, 0), (t * factor, (pack - 1 - t) * factor))) for t in range(pack)]
    )
    weights = (
        focus_scaling_vector.reshape(1, -1),
        combined_probe_matrix.T,
        sigmoid_offset_vector.reshape(-1, 1),
        focus_final_matrix,
        feedforward_scaling_vector.reshape(1, -1),
        feedforward_widen_matrix,
        feedforward_shrink_matrix,
        tensor_scaling_vector.reshape(1, -1),
        left_w,
        twin_operand_matrix[:, factor:].T,
    )
    returned, rights, pending = [], [], []
    for c in range(chunks):
        *updated, right = run_sequences(rank, arrived[c], bias, weights, heads, pack, seq_axis)
        returned += shift_all(updated)
        pending.append(right)
        if len(pending) == chunks // groups:
            right = jnp.concatenate(pending, axis=2)
            right = lax.all_to_all(right, "seq", split_axis=0, concat_axis=0, tiled=True)
            rights.append(lax.all_gather(right, "res", axis=0, tiled=True))
            pending = []
    if (seq_count // groups) % 8 != 0:
        rights = [r.transpose(1, 0, 2, 3).reshape(1, factor, -1, col_block) for r in rights]
    alignment_output, left = vmem_call(
        functools.partial(collect_kernel, chunks),
        [pieces.shape, (res_axis, chunks, rows, pack * factor)],
        rank,
        returned,
        "collect",
    )
    alignment_output = alignment_output.reshape(aligned_activity.shape)
    left = lax.all_gather(left, "seq", axis=0)
    left = left.reshape(seq_axis, res_axis, groups, chunks // groups, rows, pack, factor)
    left = left.transpose(4, 6, 2, 1, 0, 3, 5).reshape(rows * factor, -1)

    table = tensor_final_matrix.reshape(factor, factor, -1).transpose(2, 1, 0)
    table = table.reshape(table.shape[0], -1)
    pair_output = run_product(left, rights, table, pair_state)
    return (alignment_output, pair_output)


MESH = pl.DeviceIdType.MESH
GROUP = 8
AHEAD = 8
FIRST = 2
FILL = 0
UNROLL = 8
SLOW = 2
FAST = 11
LANES = 128


def dot_t(a, b):
    return dot_f32(a, b, 1, 1)


def split3(values):
    first = values.astype(jnp.bfloat16)
    rest = values - first.astype(jnp.float32)
    second = rest.astype(jnp.bfloat16)
    third = (rest - second.astype(jnp.float32)).astype(jnp.bfloat16)
    return jnp.concatenate([first, second, third], axis=0)


def wait_for(ref, sem):
    pltpu.make_async_copy(ref, ref, sem).wait()


def send(src, dst, sent, arrived, **peer):
    pltpu.make_async_remote_copy(
        src_ref=src,
        dst_ref=dst,
        send_sem=sent,
        recv_sem=arrived,
        device_id=peer,
        device_id_type=MESH,
    ).start()


class Relay:
    def __init__(self, rank, deep, wide, tile, tiles, arrived, sent_z, sent_x, forward=None):
        self.rank, self.deep, self.wide = rank, deep, wide
        self.z, self.x = rank // wide, rank % wide
        self.tile, self.tiles, self.arrived = tile, tiles, arrived
        self.sent_z, self.sent_x, self.forward = sent_z, sent_x, forward

    def pass_on(self, owner):
        for d in range(1, self.wide):
            peer = self.z * self.wide + (self.x + d) % self.wide
            send(self.tile(owner), self.tile(owner), self.sent_x, self.arrived.at[owner], res=peer)
        if self.forward is not None:
            self.forward(owner)

    def ends(self, hop, way):
        z = self.z - hop if way == 0 else self.z + hop
        there = z >= 0 if way == 0 else z < self.deep
        onward = self.z + 1 < self.deep if way == 0 else self.z >= 1
        peer = self.rank + self.wide if way == 0 else self.rank - self.wide
        return z * self.wide + self.x, there, onward, peer

    def start(self):
        for way in range(2):
            owner, _, onward, peer = self.ends(0, way)

            @pl.when(onward)
            def _():
                send(
                    self.tile(self.rank),
                    self.tile(self.rank),
                    self.sent_z.at[0, way],
                    self.arrived.at[self.rank],
                    res=peer,
                )

        self.pass_on(self.rank)

    def hop(self, hop):
        for way in range(2):
            owner, there, onward, peer = self.ends(hop, way)

            @pl.when(there)
            def _():
                wait_for(self.tile(owner), self.arrived.at[owner])

                @pl.when(onward)
                def _():
                    send(
                        self.tile(owner),
                        self.tile(owner),
                        self.sent_z.at[hop, way],
                        self.arrived.at[owner],
                        res=peer,
                    )

                self.pass_on(owner)

    def across(self):
        for d in range(1, self.wide):
            for z in range(self.deep):
                owner = z * self.wide + (self.x + d) % self.wide
                wait_for(self.tile(owner), self.arrived.at[owner])
                if self.forward is not None:
                    self.forward(owner)

    def finish(self):
        for hop in range(self.deep):
            for way in range(2):
                owner, there, onward, _ = self.ends(hop, way)

                @pl.when(jnp.logical_and(there, onward))
                def _():
                    wait_for(self.tile(owner), self.sent_z.at[hop, way])

        for d in range(1, self.wide):
            wait_for(self.tiles(self.deep), self.sent_x)


def fused_kernel(heads, ranks, wide, x_ref, pair_ref, *refs):
    given, refs = refs[:12], refs[12:]
    (out_ref, pair_out_ref), refs = refs[:2], refs[2:]
    held, refs = refs[:12], refs[12:]
    (
        gain_ref,
        probe_rows,
        offset_row,
        final_ref,
        ff_gain_ref,
        widen_ref,
        shrink_ref,
        opm_gain_ref,
        twin_ref,
        pair_gain_ref,
        pair_w_ref,
        table_rows,
    ) = held
    (
        xbuf,
        pairv,
        early,
        tile_s,
        tiles,
        bias,
        acc,
        left_acc,
        stage,
        right_v,
        left_out,
        left_in,
        left_s,
        left_t,
        normal,
        left_v,
        stack,
        probe_ref,
        offset_ref,
        table_s,
        table_ref,
    ), sems = refs[:21], refs[21:]
    (
        pair_sem,
        held_sem,
        x_in,
        x_out,
        ret_in,
        ret_out,
        tile_in,
        tile_z,
        tile_x,
        twin_out,
        twin_in,
        right_in,
        right_z,
        right_x,
        half_out,
        half_in,
        half_own,
        left_sem,
    ) = sems
    rank = lax.axis_index("res")
    core = lax.axis_index("seq")
    blocks, steps, rows, width = xbuf.shape
    length = blocks * rows
    depth = width // heads
    factor = twin_ref.shape[0] // 2
    cols = length // 2
    spans = steps // GROUP
    deep = ranks // wide

    barrier = pltpu.get_barrier_semaphore()
    for d in range(1, blocks):
        pl.semaphore_signal(
            barrier, inc=1, device_id={"res": (rank + d) % blocks}, device_id_type=MESH
        )
    pl.semaphore_signal(barrier, inc=1, device_id={"seq": 1 - core}, device_id_type=MESH)
    pair_copy = pltpu.make_async_copy(pair_ref, pairv, pair_sem.at[0])
    pair_copy.start()
    copies = [
        pltpu.make_async_copy(given[i], held[i], held_sem.at[i]) for i in range(len(given))
    ]
    for copy in copies:
        copy.start()
    pl.semaphore_wait(barrier, blocks)

    def send_x(s):
        for d in range(1, blocks):
            to = (rank + d) % blocks
            send(x_ref.at[to * steps + s], xbuf.at[rank, s], x_out.at[0], x_in.at[s], res=to)
        pltpu.make_async_copy(x_ref.at[rank * steps + s], xbuf.at[rank, s], x_in.at[s]).start()

    def send_back(s):
        def all_to(target, arrived):
            for d in range(1, blocks):
                to = (rank + d) % blocks
                send(xbuf.at[to, s], target, ret_out.at[0], arrived, res=to)
            pltpu.make_async_copy(xbuf.at[rank, s], target, arrived).start()

        @pl.when(s < GROUP)
        def _():
            all_to(early.at[rank, s], ret_in.at[0])

        @pl.when(s >= GROUP)
        def _():
            all_to(out_ref.at[rank * steps + s], ret_in.at[1])

    for s in range(FIRST):
        send_x(s)
    for copy in copies:
        copy.wait()
    pair_copy.wait()

    scaled = split3(pair_w_ref[...])

    def tile_rows(i, carry):
        normed = split3(layer_normalize(pairv[i].astype(jnp.float32), pair_gain_ref[...]))
        parts = dot_t(scaled, normed)
        tile = jnp.zeros((heads, cols), jnp.float32)
        for a, b in ((2, 0), (1, 1), (0, 2), (1, 0), (0, 1), (0, 0)):
            tile = tile + parts[a * heads : (a + 1) * heads, b * cols : (b + 1) * cols]
        for h in range(heads):
            tile_s[h, pl.ds(i, 1), :] = tile[h : h + 1]
        return carry

    lax.fori_loop(0, rows, tile_rows, 0, unroll=UNROLL)
    pack = LANES // rows
    for p in range(heads // pack):
        both = tile_s[p * pack : (p + 1) * pack].reshape(LANES, cols)
        tiles[core, rank, p] = both.T.astype(jnp.bfloat16)

    def to_twin(owner):
        send(
            tiles.at[core, owner], tiles.at[core, owner], twin_out.at[0], twin_in.at[0], seq=1 - core
        )

    spread = Relay(
        rank,
        deep,
        wide,
        lambda o: tiles.at[core, o],
        lambda c: tiles.at[core, pl.ds(0, c)],
        tile_in,
        tile_z,
        tile_x.at[0],
        to_twin,
    )

    def prepare():
        for c in range(0, probe_rows.shape[1], width):
            columns = probe_rows[:, c : c + width].astype(jnp.float32)
            probe_ref[c : c + width] = columns.T.astype(jnp.bfloat16)
        offset_ref[...] = jnp.broadcast_to(offset_row[...], (LANES, width)).T
        table_s[...] = table_rows[...].astype(jnp.float32)
        few = LANES // factor
        for e in range(0, factor, few):
            lines = [table_s[pl.ds(e + i, factor, stride=factor), :] for i in range(few)]
            lines = jnp.concatenate(lines, axis=0)
            table_ref[:, e * factor : (e + few) * factor] = lines.T.astype(jnp.bfloat16)

    spread.start()
    send_x(FIRST)
    prepare()
    for hop in range(1, deep):
        spread.hop(hop)
        if FIRST + hop < AHEAD:
            send_x(FIRST + hop)
    for s in range(min(FIRST + deep, AHEAD), AHEAD - 1):
        send_x(s)
    spread.across()
    send_x(AHEAD - 1)
    wait_for(tiles.at[1 - core], twin_in.at[0])

    low = lax.broadcasted_iota(jnp.int32, (cols, LANES), 1) < rows

    def fill(step, carry):
        half, p = step // (heads // pack), step % (heads // pack)
        for k in range(blocks // pack):
            even = tiles[half, pack * k, p].astype(jnp.float32) * LOG2E
            odd = tiles[half, pack * k + 1, p].astype(jnp.float32) * LOG2E
            here = (pl.ds(pl.multiple_of(half * cols, cols), cols), slice(k * LANES, (k + 1) * LANES))
            bias[(pack * p,) + here] = jnp.where(low, even, pltpu.roll(odd, rows, 1))
            bias[(pack * p + 1,) + here] = jnp.where(low, pltpu.roll(even, rows, 1), odd)
        return carry

    lax.fori_loop(0, 2 * heads // pack, fill, 0)

    def relay_of(u):
        return Relay(
            rank,
            deep,
            wide,
            lambda o: right_v.at[:, u, o],
            lambda c: right_v.at[:, u, pl.ds(0, c)],
            right_in.at[u],
            right_z.at[u],
            right_x.at[u],
        )

    def swap_halves(u):
        send(stage.at[u, 1], right_v.at[core, u, rank], half_out.at[u], half_in.at[u], seq=1 - core)
        pltpu.make_async_copy(stage.at[u, 0], right_v.at[core, u, rank], half_own.at[u]).start()

    def start_right(u):
        wait_for(right_v.at[core, u, rank], half_own.at[u])
        wait_for(right_v.at[1 - core, u, rank], half_in.at[u])
        relay_of(u).start()

    def due(s):
        early = steps - AHEAD
        slow = early * SLOW // 10
        return jnp.where(s <= early, s * SLOW // 10, slow + (s - early) * FAST // 10)

    def send_back_upto(first, end):
        def one(s, carry):
            send_back(s)
            return carry

        lax.fori_loop(first, end, one, 0)

    ones = jnp.ones((16, length), jnp.bfloat16)

    def sequence(s, carry):
        wait_for(xbuf.at[:, s], x_in.at[s])

        @pl.when(s + AHEAD < steps)
        def _():
            send_x(s + AHEAD)

        u, place = s // GROUP - 1, s % GROUP

        @pl.when(jnp.logical_and(u >= 0, place == 0))
        def _():
            swap_halves(u)

        send_back_upto(due(s), due(s + 1))

        @pl.when(jnp.logical_and(u >= 0, place == 1))
        def _():
            start_right(u)

        @pl.when(jnp.logical_and(u >= 0, jnp.logical_and(place > 1, place % 2 == 1)))
        def _():
            relay_of(u).hop(place // 2)

        x = xbuf[:, s].astype(jnp.float32).reshape(length, width)
        normed = layer_normalize(x, gain_ref[...]).astype(jnp.bfloat16)
        mapped = dot_t(probe_ref[...], normed)
        q = (mapped[:width] * (depth ** (-0.5) * LOG2E)).astype(jnp.bfloat16)
        k = mapped[width : 2 * width].astype(jnp.bfloat16)
        v = mapped[2 * width : 3 * width].astype(jnp.bfloat16)
        gate = jax.nn.sigmoid(mapped[3 * width :] + offset_ref[:, :1])
        gated = []
        for h in range(heads):
            part = slice(h * depth, (h + 1) * depth)
            scores = dot_f32(k[part], q[part], 0, 0) + bias[h]
            top = jnp.max(scores, axis=0, keepdims=True)
            p = jnp.exp2(scores - top).astype(jnp.bfloat16)
            mixed = dot_f32(jnp.concatenate([v[part], ones], axis=0), p, 1, 0)
            share = mixed[:depth] / mixed[depth : depth + 1]
            gated.append((share * gate[part]).astype(jnp.bfloat16))
        gated = jnp.concatenate(gated, axis=0)
        stream = x + dot_f32(gated, final_ref[...], 0, 0)
        normed = layer_normalize(stream, ff_gain_ref[...]).astype(jnp.bfloat16)
        hidden = jnp.maximum(dot_f32(normed, widen_ref[...], 1, 0), 0.0).astype(jnp.bfloat16)
        stream = stream + dot_f32(hidden, shrink_ref[...], 1, 0)
        updated = stream.astype(jnp.bfloat16)
        xbuf[:, s] = stream.reshape(blocks, rows, width).astype(jnp.bfloat16)
        normed = layer_normalize(updated.astype(jnp.float32), opm_gain_ref[...]).astype(jnp.bfloat16)
        factors = dot_t(twin_ref[...], normed)
        for e in range(factor):
            left_acc[e, pl.ds(place, 1), :] = factors[e : e + 1]
            acc[e, pl.ds(place, 1), :] = factors[factor + e : factor + e + 1]

        @pl.when(place == GROUP - 1)
        def _():
            own = pl.ds(pl.multiple_of(core * cols, cols), cols)
            other = pl.ds(pl.multiple_of((1 - core) * cols, cols), cols)
            stage[u + 1, 0] = acc[:, :, own].astype(jnp.bfloat16)
            stage[u + 1, 1] = acc[:, :, other].astype(jnp.bfloat16)

        return carry

    lax.fori_loop(0, steps, sequence, 0)

    last = spans - 1
    sent = due(steps)
    swap_halves(last)
    pairs = factor // 2
    near = lax.broadcasted_iota(jnp.int32, (pairs, GROUP, LANES), 2) < rows
    for m in range(blocks // 2):
        lanes = slice(m * LANES, (m + 1) * LANES)
        one, two = left_acc[:pairs, :, lanes], left_acc[pairs:, :, lanes]
        left_out[2 * m] = jnp.where(near, one, pltpu.roll(two, rows, 2)).astype(jnp.bfloat16)
        left_out[2 * m + 1] = jnp.where(near, pltpu.roll(one, rows, 2), two).astype(jnp.bfloat16)
    start_right(last)
    for d in range(1, blocks):
        to = (rank + d) % blocks
        send(left_out.at[to], left_in.at[rank], left_sem.at[0], left_sem.at[1], res=to)
    pltpu.make_async_copy(left_out.at[rank], left_in.at[rank], left_sem.at[1]).start()

    def normalize(b, carry):
        values = early[b].astype(jnp.float32).reshape(-1, width)
        values = layer_normalize(values, opm_gain_ref[...]).astype(jnp.bfloat16)
        place = pl.ds(pl.multiple_of(b * GROUP * rows, GROUP * rows), GROUP * rows)
        for c in range(width // LANES):
            lanes = values[:, c * LANES : (c + 1) * LANES]
            normal[c, place, :] = lanes.astype(jnp.float32)
        return carry

    def left_rows(i, carry):
        values = [
            normal[c, pl.ds(i, blocks * GROUP, stride=rows), :].astype(jnp.bfloat16)
            for c in range(width // LANES)
        ]
        values = dot_t(twin_ref[:factor], jnp.concatenate(values, axis=1))
        left_s[pl.ds(pl.multiple_of(i * factor, factor), factor), : LANES // 2] = values
        return carry

    def early_left():
        wait_for(early, ret_in.at[0])
        for b in range(blocks):
            target = out_ref.at[pl.ds(b * steps, GROUP)]
            pltpu.make_async_copy(early.at[b], target, ret_in.at[2]).start()
        lax.fori_loop(0, blocks, normalize, 0)
        lax.fori_loop(0, rows, left_rows, 0, unroll=8)

    for hop in range(1, deep):
        relay_of(last).hop(hop)
        send_back_upto(sent + (hop - 1) * FILL, sent + hop * FILL)
    send_back_upto(sent + (deep - 1) * FILL, steps)
    early_left()

    wait_for(left_in, left_sem.at[1])
    for c in range(pairs):
        values = left_in[:, c].astype(jnp.float32).reshape(blocks * GROUP, LANES).T
        values = jnp.concatenate([values, values], axis=1)
        for half in range(2):
            part = values[half * rows : (half + 1) * rows]
            left_t[pl.ds(half * pairs + c, rows, stride=factor), :] = part
    first = lax.broadcasted_iota(jnp.int32, left_s.shape, 1) < LANES // 2
    left_v[core] = jnp.where(first, left_s[...], left_t[...]).astype(jnp.bfloat16)
    send(left_v.at[core], left_v.at[core], left_sem.at[2], left_sem.at[3], seq=1 - core)
    for u in range(spans):
        relay_of(u).across()
    wait_for(left_v.at[1 - core], left_sem.at[3])

    some = stack.shape[0]
    scale = 1.0 / (2 * blocks * steps)

    def pair_block(b, carry):
        place = pl.ds(pl.multiple_of(b * some * factor, some * factor), some * factor)
        left = jnp.concatenate([left_v[0, place, :], left_v[1, place, :]], axis=1)
        for e in range(factor):
            right = right_v[:, :, :, e].reshape(2 * blocks * steps, cols)
            outer = (dot_f32(left, right, 1, 0) * scale).astype(jnp.bfloat16)
            stack[:, e * factor : (e + 1) * factor, :] = outer.reshape(some, factor, cols)
        for i in range(some):
            update = dot_f32(table_ref[...], stack[i], 1, 0)
            at = b * some + i
            pairv[at] = (pairv[at].astype(jnp.float32) + update.T).astype(jnp.bfloat16)
        these = pl.ds(b * some, some)
        pltpu.make_async_copy(pairv.at[these], pair_out_ref.at[these], pair_sem.at[1]).start()
        return carry

    lax.fori_loop(0, rows // some, pair_block, 0)

    wait_for(x_ref.at[pl.ds(0, (blocks - 1) * steps)], x_out.at[0])
    wait_for(out_ref.at[pl.ds(0, (blocks - 1) * steps)], ret_out.at[0])
    spread.finish()
    wait_for(tiles.at[core], twin_out.at[0])
    for u in range(spans):
        relay_of(u).finish()
        wait_for(stage.at[u, 1], half_out.at[u])
    wait_for(left_out.at[pl.ds(0, blocks - 1)], left_sem.at[0])
    wait_for(left_v.at[core], left_sem.at[2])
    wait_for(out_ref.at[pl.ds(0, blocks * (steps - GROUP))], ret_in.at[1])
    wait_for(early, ret_in.at[2])
    wait_for(pairv, pair_sem.at[1])


def run_fused(x, pair, weights, heads, ranks, wide):
    sequences, rows, width = x.shape
    steps = sequences // ranks
    length = rows * ranks
    cols = pair.shape[1]
    factor = weights[8].shape[0] // 2
    spans = steps // GROUP
    deep = ranks // wide
    pack = LANES // rows
    table = weights[11].shape
    any_spec = pl.BlockSpec(memory_space=pl.ANY)
    dma = lambda *shape: pltpu.SemaphoreType.DMA(shape)
    half = lambda *shape: pltpu.VMEM(shape, jnp.bfloat16)
    full = lambda *shape: pltpu.VMEM(shape, jnp.float32)
    return pl.pallas_call(
        functools.partial(fused_kernel, heads, ranks, wide),
        in_specs=[any_spec] * (2 + len(weights)),
        out_specs=[any_spec] * 2,
        out_shape=[jax.ShapeDtypeStruct(a, jnp.bfloat16) for a in (x.shape, pair.shape)],
        scratch_shapes=[pltpu.VMEM(a.shape, a.dtype) for a in weights]
        + [
            half(ranks, steps, rows, width),
            half(*pair.shape),
            half(ranks, GROUP, rows, width),
            full(heads, rows, cols),
            half(2, ranks, heads // pack, cols, LANES),
            full(heads, length, length),
            full(factor, GROUP, length),
            full(factor, GROUP, length),
            half(spans, 2, factor, GROUP, cols),
            half(2, spans, ranks, factor, GROUP, cols),
            half(ranks, factor // 2, GROUP, LANES),
            half(ranks, factor // 2, GROUP, LANES),
            full(rows * factor, LANES),
            full(rows * factor, LANES),
            full(width // LANES, ranks * GROUP * rows, LANES),
            half(2, rows * factor, LANES),
            half(math.gcd(rows, 8), factor * factor, cols),
            half(4 * width, width),
            full(width, LANES),
            full(*table),
            half(table[1], table[0]),
            dma(2),
            dma(len(weights)),
            dma(steps),
            dma(1),
            dma(3),
            dma(1),
            dma(ranks),
            dma(deep, 2),
            dma(1),
            dma(1),
            dma(1),
            dma(spans, ranks),
            dma(spans, deep, 2),
            dma(spans),
            dma(spans),
            dma(spans),
            dma(spans),
            dma(4),
        ],
        compiler_params=pltpu.CompilerParams(
            vmem_limit_bytes=FUSED_VMEM, collective_id=0, has_side_effects=True
        ),
        name="fused",
    )(x, pair, *weights)


def fits(rows, steps, ranks, heads, channels, seq_axis):
    return (
        seq_axis == 2
        and rows * 2 == LANES
        and heads == 8
        and channels == LANES
        and ranks % 2 == 0
        and steps == 2 * GROUP
        and ranks == GROUP
        and steps >= AHEAD
    )


def fused_on_device(
    aligned_activity,
    pair_state,
    focus_scaling_vector,
    combined_probe_matrix,
    sigmoid_offset_vector,
    focus_final_matrix,
    pair_norm_gain,
    pair_bias_matrix,
    feedforward_scaling_vector,
    feedforward_widen_matrix,
    feedforward_shrink_matrix,
    tensor_scaling_vector,
    twin_operand_matrix,
    tensor_final_matrix,
):
    heads = pair_bias_matrix.shape[1]
    weights = (
        focus_scaling_vector.reshape(1, -1),
        combined_probe_matrix,
        sigmoid_offset_vector.reshape(1, -1),
        focus_final_matrix,
        feedforward_scaling_vector.reshape(1, -1),
        feedforward_widen_matrix,
        feedforward_shrink_matrix,
        tensor_scaling_vector.reshape(1, -1),
        twin_operand_matrix.T,
        pair_norm_gain.reshape(1, -1),
        pair_bias_matrix.T,
        tensor_final_matrix,
    )
    return tuple(
        run_fused(aligned_activity, pair_state, weights, heads, lax.axis_size("res"), 2)
    )


def on_device(aligned_activity, pair_state, *parameters):
    ranks = lax.axis_size("res")
    rows = aligned_activity.shape[1]
    steps = aligned_activity.shape[0] // ranks
    heads = parameters[5].shape[1]
    if fits(rows, steps, ranks, heads, pair_state.shape[2], lax.axis_size("seq")):
        return fused_on_device(aligned_activity, pair_state, *parameters)
    return permuted_on_device(aligned_activity, pair_state, *parameters)


def solution(mesh):
    return jax.shard_map(
        on_device,
        mesh=mesh,
        in_specs=(
            P(("grp", "seq"), "res", None),
            P(("grp", "res"), "seq", None),
            P(),
            P(),
            P(),
            P(),
            P(),
            P(),
            P(),
            P(),
            P(),
            P(),
            P(),
            P(),
        ),
        out_specs=(P(("grp", "seq"), "res", None), P(("grp", "res"), "seq", None)),
        check_vma=False,
    )
```
